32 devices in a mesh: groups: 2 (over y), users: 4 (over z), routers: 2 (over x), heads: 2 (over core).
Axes of the slice: x: 2, y: 2, z: 4, core: 2. Of those that a mesh axis runs over, the one named last changes fastest.
Arguments:
- items: bfloat16 [64, 64, 1024], P(('groups', 'users', 'routers')), parts along dimension 0, may hold values from -6 to 6
- block_owner: int32 [64, 1], P(('groups', 'users', 'routers')), parts along dimension 0, may hold values from 0 to 3; in each aligned block of 4 rows (0 to 3, 4 to 7, ...) at most 2 rows name the same one
- block_user: int32 [64], P(('groups', 'users', 'routers')), parts along dimension 0, may hold values from 0 to 1
- block_fill: int32 [64], P(('groups', 'users', 'routers')), parts along dimension 0, may hold values from 1 to 64
- prefix_keys: bfloat16 [16, 256, 1024], P(('groups', 'users'), None, 'heads'), parts along dimension 0, may hold values from -6 to 6
- prefix_values: bfloat16 [16, 256, 1024], P(('groups', 'users'), None, 'heads'), parts along dimension 0, may hold values from -6 to 6
- w_in: bfloat16 [4, 1024, 1024], P(None, 'routers', 'heads'), may hold values from -0.1875 to 0.1875
- attn_gain: bfloat16 [1024], P('heads'), may hold values from 0.25 to 1.75
- w_o: bfloat16 [1024, 1024], P('heads', 'routers'), may hold values from -0.1875 to 0.1875
- mlp_gain: bfloat16 [1024], replicated, may hold values from 0.25 to 1.75
- w_one: bfloat16 [1024, 256], replicated, may hold values from -0.1875 to 0.1875
- w_two: bfloat16 [256], replicated, may hold values from -0.375 to 0.375
Outputs:
- scores: float32 [64, 64], P(('groups', 'users', 'routers')), parts along dimension 0
The draws below stay inside these ranges and needn't reach their ends.
There are 2 independent parts, one for each index of `groups`. The reference program is written for one: setup_inputs(seed, part) draws one part's arguments, and reference() takes and returns one part's arrays. A program takes and returns all parts, laid end to end along the dimension named above; an argument that names none is the same for every part. Nothing has to cross between parts.
Inputs may be any that keep to these rules, and one draw needn't show every extreme that they name: `block_owner`: within the rows of one device (aligned blocks of 4 blocks), no owner is named by more than 2 rows, and in every draw some owner is named by exactly 2 rows of some device.
All inputs are finite; a program needn't handle non-finite values.
Results may differ from the reference program's by a relative error of at most 0.005.
Values may be sent and summed in bfloat16 or wider, within the bound.
A program may use at most 64 MiB of HBM per device.

```python
import math
import jax
import jax.numpy as jnp
import numpy as np
from jax import lax

D = 1024
HEADS = 8
HEAD_DIM = 128
HID = 256
BLOCK = 64
CAP = 2
LPRE = 256
USR_DEV = 2
BLK_DEV = 4
HD = 1024
USERS = 8
NBLK = 32
N_USERS = 4


def touch_ends(drawn, own_key, smallest, largest):
    index_at = [jax.random.randint(jax.random.fold_in(own_key, axis), (), 0, length) for axis, length in enumerate(drawn.shape)]
    widest = drawn.shape.index(max(drawn.shape))
    beside = index_at[:widest] + [(index_at[widest] + 1) % drawn.shape[widest]] + index_at[widest + 1:]
    return drawn.at[tuple(index_at)].set(smallest).at[tuple(beside)].set(largest)


def block_scale(rng, dims, split, least, top_value):
    factor_of = 1.0
    for position, shards_of in split:
        draws = jax.random.uniform(jax.random.fold_in(jax.random.fold_in(rng, 6), position), (shards_of,), jnp.float32, least / len(split), top_value / len(split))
        factor_of = factor_of * jnp.repeat(jnp.exp(draws), dims[position] // shards_of).reshape((-1,) + (1,) * (len(dims) - 1 - position))
    return factor_of


def assign_block(rng, own, number, rows, amount, top, limit, skew):
    ranking = jax.random.permutation(rng, amount)
    crowded, ordinary = portions_of(amount, rows * top, limit, skew, True), portions_of(amount, rows * top, limit, skew, False)
    places = jnp.arange(amount)

    def named(tallies, offset_by):
        used = int((tallies > 0).sum())
        fixed = max(1, used // 4)
        passed = fixed + (places - fixed + offset_by * (used - fixed)) % max(1, amount - fixed)
        return jnp.zeros((amount,), jnp.int32).at[ranking[jnp.where(places < fixed, places, passed)]].set(jnp.asarray(tallies, jnp.int32))

    tallies = jnp.where(number % 4 == 0, named(crowded, number // 4), named(ordinary, number - number // 4 - 1))
    mixed = jax.random.permutation(jax.random.fold_in(own, 3), amount)
    source_of, sink = mixed[0:amount // 2 * 2:2], mixed[1:amount // 2 * 2:2]
    slack = jnp.minimum(tallies[source_of] - 1, limit - tallies[sink]) // 2
    slack = jnp.where((source_of == ranking[0]) | (sink == ranking[0]) | (tallies[sink] == 0), 0, jnp.maximum(slack, 0))
    passed = jax.random.randint(jax.random.fold_in(own, 4), (amount // 2,), 0, 1 << 20) % (slack + 1)
    tallies = tallies.at[source_of].add(-passed).at[sink].add(passed)
    items = jnp.searchsorted(jnp.cumsum(tallies), jnp.arange(rows * top), side="right").astype(jnp.int32)
    listing = items.reshape(top, rows).T
    listing = listing[jax.random.permutation(jax.random.fold_in(own, 1), rows)]
    offset_by = jax.random.randint(jax.random.fold_in(own, 2), (rows, 1), 0, top)
    return jnp.take_along_axis(listing, (jnp.arange(top)[None, :] + offset_by) % top, axis=1)


def portions_of(number_of, total, reach, lean, full):
    portions = [(1 << 20) // math.isqrt(rank ** lean) + 1 for rank in range(1, number_of + 1)]
    largest = reach if full else min(reach, max(-(-total // number_of), total * portions[0] // sum(portions)))
    least = 1 if total - largest >= number_of - 1 else 0
    counts, rest = [largest] + [least] * (number_of - 1), total - largest - least * (number_of - 1)
    while rest > 0:
        movable = [i for i in range(1, number_of) if counts[i] < largest] or [i for i in range(1, number_of) if counts[i] < reach]
        pool, remaining = sum([portions[i] for i in movable]), rest
        for i in movable:
            addition = min(reach - counts[i], max(1, remaining * portions[i] // pool), rest)
            counts[i] = counts[i] + addition
            rest = rest - addition
    return np.array(counts)


def gaussian(rng, dims, scale, most, shards=(), held_as=jnp.bfloat16):
    gain = block_scale(rng, dims, shards, -0.22, 0.18) if shards else 1.0
    values = jax.random.normal(rng, dims, jnp.float32) * scale * gain
    return jnp.minimum(jnp.maximum(values, -most), most).astype(held_as)


def setup_inputs(seed: int = 0, part: int = 0) -> dict:
    seeds = jax.random.split(jax.random.key(seed), 13)
    part_splits = jax.random.split(jax.random.fold_in(seeds[12], part), 13)
    items = gaussian(part_splits[0], (NBLK, BLOCK, D), 1.0, 6.0, ((0, 8),))
    block_owner_keys = jax.random.split(jax.random.fold_in(part_splits[1], 1), NBLK // BLK_DEV)
    block_owner_turns = jax.random.permutation(jax.random.fold_in(part_splits[1], 3), NBLK // BLK_DEV)
    block_owner = jax.vmap(lambda own, number: assign_block(jax.random.fold_in(part_splits[1], 2), own, number, BLK_DEV, N_USERS, 1, CAP, 2))(block_owner_keys, block_owner_turns).reshape((NBLK, 1))
    block_user = touch_ends(jax.random.randint(part_splits[2], (NBLK,), 0, USR_DEV), jax.random.fold_in(part_splits[2], 1), 0, USR_DEV - 1).astype(jnp.int32)
    block_fill = touch_ends(jax.random.randint(part_splits[3], (NBLK,), 1, BLOCK + 1), jax.random.fold_in(part_splits[3], 1), 1, BLOCK).astype(jnp.int32)
    prefix_keys = gaussian(part_splits[4], (USERS, LPRE, HD), 1.0, 6.0, ((0, 4), (2, 2)))
    prefix_values = gaussian(part_splits[5], (USERS, LPRE, HD), 1.0, 6.0, ((0, 4), (2, 2)))
    w_in = gaussian(seeds[6], (4, D, HD), D ** -0.5, 0.1875, ((1, 2), (2, 2)))
    attn_gain = jnp.clip(1.0 + 0.15 * jax.random.normal(seeds[7], (HD,), jnp.float32), 0.25, 1.75).astype(jnp.bfloat16)
    w_o = gaussian(seeds[8], (HD, D), HD ** -0.5, 0.1875, ((0, 2), (1, 2)))
    mlp_gain = jnp.clip(1.0 + 0.15 * jax.random.normal(seeds[9], (D,), jnp.float32), 0.25, 1.75).astype(jnp.bfloat16)
    w_one = gaussian(seeds[10], (D, HID), D ** -0.5, 0.1875)
    w_two = gaussian(seeds[11], (HID,), HID ** -0.5, 0.375)
    return dict(items=items, block_owner=block_owner, block_user=block_user, block_fill=block_fill, prefix_keys=prefix_keys, prefix_values=prefix_values, w_in=w_in, attn_gain=attn_gain, w_o=w_o, mlp_gain=mlp_gain, w_one=w_one, w_two=w_two)


def score_block(block_items, owner_index, user_index, fill_count, prefix_keys, prefix_values, wide_in, attn_gain, w_o, mlp_gain, w_one, w_two):
    score_scale = HEAD_DIM ** (-0.5)
    cache_slot = (owner_index * USR_DEV + user_index).astype(jnp.int32)
    user_keys = lax.dynamic_index_in_dim(prefix_keys, cache_slot, 0, keepdims=False)
    user_values = lax.dynamic_index_in_dim(prefix_values, cache_slot, 0, keepdims=False)
    projected = jax.nn.silu(jnp.einsum('rk,pkc->prc', block_items.astype(jnp.float32), wide_in))
    queries = projected[0].astype(jnp.bfloat16)
    query_heads = queries.astype(jnp.float32).reshape(BLOCK, HEADS, HEAD_DIM)
    key_heads = user_keys.astype(jnp.float32).reshape(LPRE, HEADS, HEAD_DIM)
    value_heads = user_values.astype(jnp.float32).reshape(LPRE, HEADS, HEAD_DIM)
    raw_scores = jnp.einsum('qhd,khd->hqk', query_heads, key_heads) * score_scale
    weights = jax.nn.silu(raw_scores).astype(jnp.bfloat16)
    prefix_part = jnp.einsum('hqk,khd->qhd', weights.astype(jnp.float32), value_heads).astype(jnp.bfloat16)
    self_keys = projected[1].reshape(BLOCK, HEADS, HEAD_DIM)
    self_values = projected[2].reshape(BLOCK, HEADS, HEAD_DIM)
    gates = projected[3]
    own_term = jax.nn.silu(lax.optimization_barrier(jnp.sum(query_heads * self_keys, axis=-1)) * score_scale)[..., None] * self_values
    attended = (prefix_part.astype(jnp.float32) + own_term).reshape(BLOCK, HD)
    row_mean = lax.optimization_barrier(jnp.sum(attended, axis=1)) / HD
    row_var = lax.optimization_barrier(jnp.sum(attended * attended, axis=1)) / HD - row_mean * row_mean
    gated = ((attended - row_mean[:, None]) * lax.rsqrt(row_var + 1e-05)[:, None] * attn_gain.astype(jnp.float32) * gates).astype(jnp.bfloat16)
    residual = block_items.astype(jnp.float32) + jnp.dot(gated, w_o, preferred_element_type=jnp.float32)
    row_scale = lax.rsqrt(lax.optimization_barrier(jnp.sum(residual * residual, axis=1)) / D + 1e-05)
    normed = (residual * row_scale[:, None] * mlp_gain.astype(jnp.float32)).astype(jnp.bfloat16)
    hidden = jax.nn.silu(jnp.dot(normed, w_one, preferred_element_type=jnp.float32)).astype(jnp.bfloat16)
    block_scores = jnp.dot(hidden, w_two, preferred_element_type=jnp.float32)
    is_valid = jnp.arange(BLOCK, dtype=jnp.int32) < fill_count
    return jnp.where(is_valid, block_scores, jnp.zeros_like(block_scores))

def reference(items, block_owner, block_user, block_fill, prefix_keys, prefix_values, w_in, attn_gain, w_o, mlp_gain, w_one, w_two):
    wide_in = w_in.astype(jnp.float32)

    def one_block(packed):
        block_items, owner_index, user_index, fill_count = packed
        return score_block(block_items, owner_index, user_index, fill_count, prefix_keys, prefix_values, wide_in, attn_gain, w_o, mlp_gain, w_one, w_two)
    return lax.map(one_block, (items, block_owner[:, 0], block_user, block_fill))
```

```python
import functools
import math

import jax
import jax.numpy as jnp
from jax import lax
from jax.experimental import pallas as pl
from jax.experimental.pallas import tpu as pltpu
from jax.sharding import PartitionSpec as P

HEAD_DIM = 128
CAP = 2
EPSILON = 1e-05
TREE_EIGHTHS = (0, 5, 5, 5, 4)
PARTS = (4, 1, 1, 1, 4)
ORDER = (
    [(0, "g", part) for part in range(PARTS[0])]
    + [(1, "t", 0), (2, "t", 0), (1, "g", 0), (3, "t", 0), (4, "t", 0), (2, "g", 0), (3, "g", 0)]
    + [(4, "g", part) for part in range(PARTS[4])]
)
F32 = jnp.float32
BF16 = jnp.bfloat16
MESH = pl.DeviceIdType.MESH


def silu(v):
    return 0.5 * v * (1.0 + jnp.tanh(0.5 * v))


def scorer(
    sizes,
    items_ref,
    owner_hbm,
    user_hbm,
    fill_hbm,
    keys_ref,
    values_ref,
    w_in_ref,
    attn_gain_hbm,
    w_o_ref,
    mlp_gain_hbm,
    w_one_ref,
    w_two_hbm,
    out_ref,
    owner_ref,
    user_ref,
    fill_ref,
    attn_gain_ref,
    mlp_gain_ref,
    w_two_ref,
    items_v,
    out_slots,
    x_all,
    mask_out,
    mask_all,
    keys_v,
    values_v,
    w_all,
    wo_all,
    w_one_v,
    q_v,
    own_v,
    att_v,
    gated_v,
    stat_out,
    stat_in,
    part_out,
    part_own,
    part_in,
    sc_out,
    ret,
    local_sem,
    sent,
    z_recv,
    group_recv,
    x_recv,
    y_recv,
    w_recv,
    po_recv,
    sc_send,
    sc_recv,
    yard,
):
    groups, users, routers, heads = sizes
    g = lax.axis_index("groups")
    me = lax.axis_index("users")
    r = lax.axis_index("routers")
    h = lax.axis_index("heads")
    mate = 1 - h
    blocks, width, model = items_v.shape
    slots = x_all.shape[0]
    half_width = q_v.shape[1]
    heads_here = half_width // HEAD_DIM
    hd_all = half_width * heads
    rows = slots * width
    depth = w_all.shape[2]
    out_cols = wo_all.shape[2]
    wh = width // heads
    scale = HEAD_DIM ** (-0.5)
    positions = keys_v.shape[0] * keys_v.shape[1]
    per_user = keys_v.shape[1]

    barrier = pltpu.get_barrier_semaphore()
    count = 0
    for j in range(1, routers):
        pl.semaphore_signal(
            barrier, inc=1, device_id={"routers": lax.rem(r + j, routers)}, device_id_type=MESH
        )
        count += 1
    for i in range(1, groups):
        pl.semaphore_signal(
            barrier, inc=1, device_id={"groups": lax.rem(g + i, groups)}, device_id_type=MESH
        )
        count += 1
    pl.semaphore_signal(barrier, inc=1, device_id={"heads": mate}, device_id_type=MESH)
    count += 1
    for k in range(1, users):
        for e in range(heads):
            pl.semaphore_signal(
                barrier,
                inc=1,
                device_id={"users": lax.rem(me + k, users), "heads": e},
                device_id_type=MESH,
            )
            count += 1
    first = [
        pltpu.make_async_copy(src, dst, local_sem.at[n])
        for n, (src, dst) in enumerate(
            (
                (owner_hbm, owner_ref),
                (user_hbm, user_ref),
                (fill_hbm, fill_ref),
                (items_ref, items_v),
            )
        )
    ]
    gains = [
        pltpu.make_async_copy(src, dst, local_sem.at[4 + n])
        for n, (src, dst) in enumerate(
            (
                (attn_gain_hbm, attn_gain_ref),
                (mlp_gain_hbm, mlp_gain_ref),
                (w_two_hbm, w_two_ref),
            )
        )
    ]
    bulk = [
        pltpu.make_async_copy(src, dst, local_sem.at[7])
        for src, dst in (
            (w_in_ref, w_all.at[:, r]),
            (keys_ref, keys_v),
            (values_ref, values_v),
            (w_o_ref, wo_all.at[r]),
            (w_one_ref, w_one_v),
        )
    ]

    def size(*refs):
        return sum(math.prod(ref.shape) * jnp.dtype(ref.dtype).itemsize for ref in refs)

    def drain(sem, amount):
        part = yard.at[pl.ds(0, amount // (yard.shape[1] * 2)), :]
        pltpu.make_async_copy(part, part, sem).wait()

    for c in first:
        c.start()
    pl.semaphore_wait(barrier, count)

    pieces = ORDER
    number = {piece: t for t, piece in enumerate(pieces)}
    slot_y = [p if kind == "g" else 4 + p for p, kind, _ in pieces]
    parity = lax.rem(me, 2)
    pair = me + 1 - 2 * parity

    def piece_rows(p, kind, part, owner_group, owner_parity):
        length = depth if p < 4 else half_width
        tree = length * TREE_EIGHTHS[p] // 8 // (2 * groups) // 16 * 16
        if kind == "t":
            return pl.ds(pl.multiple_of((owner_group * 2 + owner_parity) * tree, tree), tree)
        direct = length // groups - 2 * tree
        share = direct // PARTS[p]
        start = 2 * groups * tree + owner_group * direct + part * share
        return pl.ds(pl.multiple_of(start, math.gcd(share, 16)), share)

    def weight_slot(owner_router, owner_group, owner_parity, t):
        p, kind, part = pieces[t]
        span = piece_rows(p, kind, part, owner_group, owner_parity)
        if p < 4:
            return w_all.at[p, owner_router, span, :]
        return wo_all.at[owner_router, span, :]

    def piece_bytes(t):
        p, kind, part = pieces[t]
        row = size(w_all) // (4 * routers * depth) if p < 4 else size(wo_all) // (routers * half_width)
        length = depth if p < 4 else half_width
        tree = length * TREE_EIGHTHS[p] // 8 // (2 * groups) // 16 * 16
        if kind == "t":
            return tree * row
        return (length // groups - 2 * tree) // PARTS[p] * row

    def x_copy(j, t, source_router):
        p, kind, part = pieces[t]
        span = piece_rows(p, kind, part, g, parity)
        src = w_in_ref.at[p, span, :] if p < 4 else w_o_ref.at[span, :]
        return pltpu.make_async_remote_copy(
            src_ref=src,
            dst_ref=weight_slot(source_router, g, parity, t),
            send_sem=sent.at[0],
            recv_sem=x_recv.at[j - 1, t],
            device_id={"routers": lax.rem(r + j, routers)},
            device_id_type=MESH,
        )

    def y_copy(i, j, t, owner_group):
        spot = weight_slot(lax.rem(r - j + routers, routers), owner_group, parity, t)
        return pltpu.make_async_remote_copy(
            src_ref=spot,
            dst_ref=spot,
            send_sem=sent.at[0],
            recv_sem=y_recv.at[i - 1, j - 1, slot_y[t]],
            device_id={"groups": lax.rem(g + i, groups)},
            device_id_type=MESH,
        )

    def pair_copy(i, j, p, owner_parity):
        spot = weight_slot(
            lax.rem(r - j + routers, routers),
            lax.rem(g - i + groups, groups),
            owner_parity,
            number[p, "t", 0],
        )
        return pltpu.make_async_remote_copy(
            src_ref=spot,
            dst_ref=spot,
            send_sem=sent.at[0],
            recv_sem=w_recv.at[j - 1, p],
            device_id={"users": pair},
            device_id_type=MESH,
        )

    for t in range(len(pieces)):
        for j in range(1, routers):
            x_copy(j, t, r).start()
    for c in bulk + gains:
        c.start()

    for c in first[:3]:
        c.wait()
    owners = [owner_ref[b] for b in range(blocks)]
    ranks = []
    for b in range(blocks):
        rank = jnp.int32(0)
        for a in range(b):
            rank = rank + jnp.where(owners[a] == owners[b], 1, 0)
        ranks.append(rank)

    def slot_source(dest, cap):
        index, user = jnp.int32(0), jnp.int32(-1)
        for b in range(blocks):
            hit = (owners[b] == dest) & (ranks[b] == cap)
            index = jnp.where(hit, b, index)
            user = jnp.where(hit, user_ref[b], user)
        return index, user

    mask_bytes = size(mask_out) // users
    slot_bytes = size(out_slots) // users
    lane_user = lax.broadcasted_iota(jnp.int32, (1, positions), 1) // per_user
    mask_copies, item_copies = {}, {}

    def z_copy(k, source):
        return pltpu.make_async_remote_copy(
            src_ref=out_slots.at[k],
            dst_ref=x_all.at[pl.ds(source * CAP, CAP), pl.ds(pl.multiple_of(h * wh, wh), wh), :],
            send_sem=sent.at[0],
            recv_sem=z_recv.at[k - 1],
            device_id={"users": lax.rem(me + k, users)},
            device_id_type=MESH,
        )

    def m_copy(k, source):
        return pltpu.make_async_remote_copy(
            src_ref=mask_out.at[k],
            dst_ref=mask_all.at[source],
            send_sem=sent.at[0],
            recv_sem=group_recv.at[0],
            device_id={"users": lax.rem(me + k, users)},
            device_id_type=MESH,
        )

    def relay_copy(k, part):
        source = lax.rem(me - k + users, users)
        spot = x_all.at[pl.ds(source * CAP, CAP), pl.ds(pl.multiple_of(part * wh, wh), wh), :]
        return pltpu.make_async_remote_copy(
            src_ref=spot,
            dst_ref=spot,
            send_sem=sent.at[0],
            recv_sem=group_recv.at[1],
            device_id={"heads": mate},
            device_id_type=MESH,
        )

    first[3].wait()
    for k in list(range(1, users)) + [0]:
        dest = lax.rem(me + k, users)
        for cap in range(CAP):
            index, user = slot_source(dest, cap)
            line = jnp.where(lane_user == user, 1.0, 0.0).astype(F32)
            if k == 0:
                x_all[me * CAP + cap] = items_v[index]
                mask_all[me, cap : cap + 1, :] = line
            else:
                out_slots[k, cap] = items_v[index, pl.ds(pl.multiple_of(h * wh, wh), wh), :]
                mask_out[k, cap : cap + 1, :] = line
        if k:
            z_copy(k, me).start()
            m_copy(k, me).start()

    def forward(p, kind, part=0):
        t = number[p, kind, part]
        for j in range(1, routers):
            x_copy(j, t, lax.rem(r - j + routers, routers)).wait_recv()
            for i in range(1, groups):
                y_copy(i, j, t, g).start()
            if kind == "t":
                pair_copy(0, j, p, parity).start()

    def y_landed(p, kind):
        t = number[p, kind, 0]
        for j in range(1, routers):
            for i in range(1, groups):
                y_copy(i, j, t, lax.rem(g - i + groups, groups)).wait_recv()
                pair_copy(i, j, p, parity).start()

    def landed(p):
        for j in range(1, routers):
            for i in range(1, groups):
                drain(y_recv.at[i - 1, j - 1, p], PARTS[p] * piece_bytes(number[p, "g", 0]))
            if TREE_EIGHTHS[p]:
                drain(w_recv.at[j - 1, p], groups * piece_bytes(number[p, "t", 0]))

    tile_slots = 4
    tile = tile_slots * width
    tiles = rows // tile

    def x_tile(i):
        return x_all[pl.ds(i * tile_slots, tile_slots)].reshape(tile, model)

    def span_of(i):
        return pl.ds(pl.multiple_of(i * tile, tile), tile)

    def projected(p, i):
        x = x_tile(i)
        total = jnp.zeros((tile, half_width), F32)
        for a in range(routers):
            total = total + jnp.dot(
                x[:, a * depth : (a + 1) * depth], w_all[p, a], preferred_element_type=F32
            )
        return silu(total)

    def query(i):
        q_v[span_of(i), :] = projected(0, i).astype(BF16)

    def attend(i):
        span = span_of(i)
        for e in range(heads_here):
            cols = slice(e * HEAD_DIM, (e + 1) * HEAD_DIM)
            raw = lax.dot_general(
                q_v[span, cols],
                keys_v[:, :, cols].reshape(positions, HEAD_DIM),
                (((1,), (1,)), ((), ())),
                preferred_element_type=F32,
            )
            weights = silu(raw * scale)
            parts = []
            for s in range(tile_slots):
                line = mask_all[i * (tile_slots // CAP) + s // CAP, s % CAP : s % CAP + 1, :]
                parts.append(weights[s * width : (s + 1) * width] * line)
            weights = jnp.concatenate(parts, axis=0).astype(BF16)
            att_v[span, cols] = (
                jnp.dot(
                    weights,
                    values_v[:, :, cols].reshape(positions, HEAD_DIM),
                    preferred_element_type=F32,
                )
                .astype(BF16)
                .astype(F32)
            )

    def self_key(i):
        span = span_of(i)
        keys = projected(1, i)
        for e in range(heads_here):
            cols = slice(e * HEAD_DIM, (e + 1) * HEAD_DIM)
            own = jnp.sum(q_v[span, cols].astype(F32) * keys[:, cols], axis=1, keepdims=True)
            own_v[span, cols] = jnp.broadcast_to(silu(own * scale), (tile, HEAD_DIM))

    lane = lax.broadcasted_iota(jnp.int32, (tile, 128), 1)

    def self_value(i):
        span = span_of(i)
        att = att_v[span, :] + own_v[span, :] * projected(2, i)
        att_v[span, :] = att
        total = jnp.sum(att, axis=1, keepdims=True)
        square = jnp.sum(att * att, axis=1, keepdims=True)
        stat_out[span, :] = jnp.where(lane == 0, total, square)

    def gate(i):
        span = span_of(i)
        both = stat_out[span, :] + stat_in[span, :]
        mean = both[:, 0:1] / hd_all
        var = both[:, 1:2] / hd_all - mean * mean
        gated_v[span, :] = (
            (att_v[span, :] - mean)
            * lax.rsqrt(var + EPSILON)
            * attn_gain_ref[...].astype(F32).reshape(1, -1)
            * projected(3, i)
        ).astype(BF16)

    with jax.named_scope("fwd0"):
        for part in range(PARTS[0]):
            forward(0, "g", part)
    with jax.named_scope("fwd1"):
        forward(1, "t")
        forward(2, "t")
        forward(1, "g")
    with jax.named_scope("items"):
        for k in range(1, users):
            z_copy(k, lax.rem(me - k + users, users)).wait_recv()
            relay_copy(k, h).start()
    with jax.named_scope("fwd1b"):
        y_landed(1, "t")
    with jax.named_scope("items2"):
        drain(group_recv.at[0], (users - 1) * mask_bytes)
        drain(group_recv.at[1], (users - 1) * slot_bytes)
        drain(local_sem.at[7], size(w_in_ref, keys_ref, values_ref, w_o_ref, w_one_ref))
        for c in gains:
            c.wait()
    with jax.named_scope("land0"):
        landed(0)
    with jax.named_scope("query"):
        pl.loop(0, tiles)(query)
    with jax.named_scope("fwd3a"):
        forward(3, "t")
        y_landed(2, "t")
    with jax.named_scope("attend0"):
        pl.loop(0, tiles // 2)(attend)
    with jax.named_scope("fwd4a"):
        forward(4, "t")
    with jax.named_scope("attend1"):
        pl.loop(tiles // 2, tiles)(attend)
    with jax.named_scope("fwd2b"):
        forward(2, "g")
    with jax.named_scope("land1"):
        landed(1)
    with jax.named_scope("key"):
        pl.loop(0, tiles)(self_key)
    with jax.named_scope("fwd3b"):
        forward(3, "g")
        y_landed(3, "t")
        forward(4, "g", 0)
        y_landed(4, "t")
        forward(4, "g", 1)
    with jax.named_scope("land2"):
        landed(2)
    with jax.named_scope("value0"):
        pl.loop(0, tiles // 2)(self_value)
    with jax.named_scope("fwd4c"):
        forward(4, "g", 2)
    with jax.named_scope("value1"):
        pl.loop(tiles // 2, tiles)(self_value)

    stat_copy = pltpu.make_async_remote_copy(
        src_ref=stat_out,
        dst_ref=stat_in,
        send_sem=sent.at[0],
        recv_sem=group_recv.at[2],
        device_id={"heads": mate},
        device_id_type=MESH,
    )
    stat_copy.start()
    with jax.named_scope("fwd4b"):
        forward(4, "g", 3)
    with jax.named_scope("land3"):
        landed(3)
    with jax.named_scope("statwait"):
        stat_copy.wait_recv()
    with jax.named_scope("gate"):
        pl.loop(0, tiles)(gate)

    half = rows // heads

    mine = users // heads
    piece = half // 2
    source_rows = CAP * width

    def far_first(e, i, amount):
        return jnp.where(me < e * mine + mine // 2, amount - 1 - i, i)

    def part_copy(j, c):
        spot = pl.ds(pl.multiple_of(c * piece, piece), piece)
        return pltpu.make_async_remote_copy(
            src_ref=part_out.at[j, spot, :],
            dst_ref=part_in.at[j, spot, :],
            send_sem=sent.at[0],
            recv_sem=po_recv.at[c],
            device_id={"heads": mate},
            device_id_type=MESH,
        )

    def out_project(j, row_half, c, target):
        src = pl.ds(pl.multiple_of(row_half * half + c * piece, piece), piece)
        target[j, pl.ds(pl.multiple_of(c * piece, piece), piece), :] = jnp.dot(
            gated_v[src, :],
            wo_all[lax.rem(r - j + routers, routers)],
            preferred_element_type=F32,
        ).astype(target.dtype)

    def shares(j):
        for i in range(2):
            c = far_first(mate, i, 2)
            out_project(j, mate, c, part_out)
            part_copy(j, c).start()

    with jax.named_scope("outown"):
        shares(0)
        for c in range(2):
            out_project(0, h, c, part_own)
    with jax.named_scope("land4"):
        landed(4)
    for j in range(1, routers):
        shares(j)
    for j in range(1, routers):
        for c in range(2):
            out_project(j, h, c, part_own)

    two = jnp.broadcast_to(
        w_two_ref[...].astype(F32).reshape(1, -1), (8, w_two_ref.shape[0])
    ).astype(BF16)

    def score(source, i):
        span = pl.ds(pl.multiple_of(source * source_rows, source_rows), source_rows)
        x = x_all[pl.ds((h * mine + source) * CAP, CAP)].reshape(source_rows, model).astype(F32)
        mixed = []
        for a in range(routers):
            j = lax.rem(r - a + routers, routers)
            mixed.append(part_own[j, span, :] + part_in[j, span, :].astype(F32))
        residual = x + jnp.concatenate(mixed, axis=1)
        norm = lax.rsqrt(jnp.sum(residual * residual, axis=1, keepdims=True) / model + EPSILON)
        normed = (residual * norm * mlp_gain_ref[...].astype(F32).reshape(1, -1)).astype(BF16)
        hidden = silu(jnp.dot(normed, w_one_v[...], preferred_element_type=F32)).astype(BF16)
        sc_out[i] = lax.dot_general(
            two, hidden, (((1,), (1,)), ((), ())), preferred_element_type=F32
        )

    def score_copy(i, e, owner, sem):
        return pltpu.make_async_remote_copy(
            src_ref=sc_out.at[i],
            dst_ref=ret.at[owner],
            send_sem=sc_send.at[i, e],
            recv_sem=sc_recv.at[sem],
            device_id={"users": h * mine + far_first(h, i, mine), "heads": e},
            device_id_type=MESH,
        )

    for i in range(mine):
        source = far_first(h, i, mine)
        if i % (mine // 2) == 0:
            with jax.named_scope("partwait"):
                drain(po_recv.at[far_first(h, i // (mine // 2), 2)], size(part_in) // 2)
        score(source, i)
        target = h * mine + source
        for e in range(heads):
            itself = (target == me) & (h == e)

            @pl.when(jnp.logical_not(itself))
            def _():
                score_copy(i, e, me, me).start()

            @pl.when(itself)
            def _():
                ret[me] = sc_out[i]

    hops = sum(piece_bytes(t) * groups for t in range(len(pieces)))
    hops += sum(piece_bytes(number[p, "t", 0]) * groups for p in range(5) if TREE_EIGHTHS[p])
    total = (routers - 1) * hops + (users - 1) * (2 * slot_bytes + mask_bytes)
    drain(sent.at[0], total + size(stat_out) + size(part_out))
    handler = me // mine
    with jax.named_scope("scorewait"):
        for d in range(users):

            @pl.when(jnp.logical_not((d == me) & (h == handler)))
            def _():
                score_copy(0, 0, d, d).wait_recv()

    position = lax.broadcasted_iota(jnp.int32, (1, width), 1)
    for b in range(blocks):
        tile_in = ret[owners[b]]
        line = tile_in[0:1, 0:width]
        for cap in range(1, CAP):
            line = jnp.where(ranks[b] == cap, tile_in[0:1, cap * width : (cap + 1) * width], line)
        out_ref[b : b + 1, :] = jnp.where(position < fill_ref[b], line, 0.0)

    for i in range(mine):
        for e in range(heads):

            @pl.when(jnp.logical_not((h * mine + far_first(h, i, mine) == me) & (h == e)))
            def _():
                score_copy(i, e, me, me).wait_send()


def local(
    sizes,
    items,
    block_owner,
    block_user,
    block_fill,
    prefix_keys,
    prefix_values,
    w_in,
    attn_gain,
    w_o,
    mlp_gain,
    w_one,
    w_two,
):
    groups, users, routers, heads = sizes
    blocks, width, model = items.shape
    projections, depth, half_width = w_in.shape
    slots = users * CAP
    rows = slots * width
    half = rows // heads
    out_cols = w_o.shape[1]
    cached, per_user, _ = prefix_keys.shape
    positions = cached * per_user
    pieces = len(ORDER)
    dma = pltpu.SemaphoreType.DMA
    yard_bytes = 2 * (
        (routers - 1) * (w_in.size + w_o.size)
        + (users - 1) * (2 * CAP * (width // heads) * model + 2 * 8 * positions)
        + 2 * rows * 128
        + routers * half * out_cols
    )
    yard_rows = yard_bytes // 256 // 8 * 8
    hbm = pl.BlockSpec(memory_space=pl.ANY)
    vmem = pl.BlockSpec(memory_space=pltpu.VMEM)
    scratch = [
        pltpu.SMEM((blocks,), jnp.int32),
        pltpu.SMEM((blocks,), jnp.int32),
        pltpu.SMEM((blocks,), jnp.int32),
        pltpu.VMEM(attn_gain.shape, BF16),
        pltpu.VMEM(mlp_gain.shape, BF16),
        pltpu.VMEM(w_two.shape, BF16),
        pltpu.VMEM((blocks, width, model), BF16),
        pltpu.VMEM((users, CAP, width // heads, model), BF16),
        pltpu.VMEM((slots, width, model), BF16),
        pltpu.VMEM((users, 8, positions), F32),
        pltpu.VMEM((users, 8, positions), F32),
        pltpu.VMEM(prefix_keys.shape, BF16),
        pltpu.VMEM(prefix_values.shape, BF16),
        pltpu.VMEM((projections, routers, depth, half_width), BF16),
        pltpu.VMEM((routers, half_width, out_cols), BF16),
        pltpu.VMEM(w_one.shape, BF16),
        pltpu.VMEM((rows, half_width), BF16),
        pltpu.VMEM((rows, half_width), F32),
        pltpu.VMEM((rows, half_width), F32),
        pltpu.VMEM((rows, half_width), BF16),
        pltpu.VMEM((rows, 128), F32),
        pltpu.VMEM((rows, 128), F32),
        pltpu.VMEM((routers, half, out_cols), BF16),
        pltpu.VMEM((routers, half, out_cols), F32),
        pltpu.VMEM((routers, half, out_cols), BF16),
        pltpu.VMEM((users // heads, 8, CAP * width), F32),
        pltpu.VMEM((users, 8, CAP * width), F32),
        dma((8,)),
        dma((1,)),
        dma((users - 1,)),
        dma((3,)),
        dma((routers - 1, pieces)),
        dma((groups - 1, routers - 1, 9)),
        dma((routers - 1, 5)),
        dma((2,)),
        dma((users // heads, heads)),
        dma((users,)),
        pltpu.VMEM((yard_rows, 128), BF16),
    ]
    return pl.pallas_call(
        functools.partial(scorer, sizes),
        out_shape=pltpu.VMEM((blocks, width), F32),
        in_specs=[hbm] * 12,
        out_specs=vmem,
        scratch_shapes=scratch,
        compiler_params=pltpu.CompilerParams(
            collective_id=0, has_side_effects=True, vmem_limit_bytes=62 * 1024 * 1024
        ),
    )(
        items,
        block_owner.reshape(-1),
        block_user,
        block_fill,
        prefix_keys,
        prefix_values,
        w_in,
        attn_gain,
        w_o,
        mlp_gain,
        w_one,
        w_two,
    )


def solution(mesh):
    placed = (
        P(("groups", "users", "routers"), None, None),
        P(("groups", "users", "routers"), None),
        P(("groups", "users", "routers")),
        P(("groups", "users", "routers")),
        P(("groups", "users"), None, "heads"),
        P(("groups", "users"), None, "heads"),
        P(None, "routers", "heads"),
        P("heads"),
        P("heads", "routers"),
        P(),
        P(),
        P(),
    )
    sizes = tuple(mesh.shape[name] for name in ("groups", "users", "routers", "heads"))
    return jax.shard_map(
        functools.partial(local, sizes),
        mesh=mesh,
        in_specs=placed,
        out_specs=P(("groups", "users", "routers"), None),
        check_vma=False,
    )
```

```python
import functools
import math

import jax
import jax.numpy as jnp
from jax import lax
from jax.experimental import pallas as pl
from jax.experimental.pallas import tpu as pltpu
from jax.sharding import PartitionSpec as P

HEAD_DIM = 128
CAP = 2
EPSILON = 1e-05
UNIT = 512
PIECES = (
    (1, "t", 112),
    (0, "g", 80),
    (2, "t", 80),
    (0, "g", 80),
    (0, "g", 96),
    (3, "t", 64),
    (1, "g", 32),
    (3, "t", 32),
    (2, "g", 96),
    (3, "g", 64),
    (4, "g", 96),
    (4, "p", 32),
    (4, "p", 32),
    (4, "o", 192),
    (3, "o", 0),
    (2, "o", 0),
    (1, "o", 0),
    (0, "o", 0),
)
STEPS = (
    "T", "f0", "f1", "f2", "r1", "r2", "z0", "f3", "f4", "r3", "z2", "f5", "f6", "f7", "f8", "L0",
    "rA", "qA", "aA0", "aA1", "f9", "z5", "rB", "qB", "aB0", "z7", "aB1", "f10", "L1", "kA", "f11",
    "kB", "f12", "L2", "v0", "v1", "L3", "g0", "g1", "o0", "L4", "o1",
)
F32 = jnp.float32
BF16 = jnp.bfloat16
MESH = pl.DeviceIdType.MESH


def silu(v):
    return 0.5 * v * (1.0 + jnp.tanh(0.5 * v))


def plan(groups, depth, half_width):
    copies = {"t": groups * 2, "g": groups, "p": 2, "o": 1}
    lengths = [depth] * 4 + [half_width]
    filled = [0] * 5
    pieces = []
    for p, kind, share in PIECES:
        count = 0 if kind == "o" else share * lengths[p] // UNIT // 16 * 16
        pieces.append([p, kind, filled[p], count])
        filled[p] += copies[kind] * count
    for piece in pieces:
        p = piece[0]
        if piece[1] == "o":
            piece[2:] = filled[p], lengths[p] - filled[p]
            filled[p] = lengths[p]
    return pieces


def scorer(
    sizes,
    items_ref,
    owner_hbm,
    user_hbm,
    fill_hbm,
    keys_ref,
    values_ref,
    w_in_ref,
    attn_gain_hbm,
    w_o_ref,
    mlp_gain_hbm,
    w_one_ref,
    w_two_hbm,
    out_ref,
    owner_ref,
    user_ref,
    fill_ref,
    attn_gain_ref,
    mlp_gain_ref,
    w_two_ref,
    items_v,
    out_slots,
    x_all,
    mask_out,
    mask_all,
    keys_v,
    values_v,
    turned,
    gain_v,
    w_all,
    wo_all,
    w_one_v,
    q_v,
    own_v,
    att_v,
    gated_v,
    stat_out,
    stat_in,
    part_out,
    part_own,
    part_in,
    sc_out,
    ret,
    local_sem,
    sent,
    z_recv,
    group_recv,
    x_recv,
    y_recv,
    w_recv,
    st_recv,
    po_recv,
    sc_send,
    sc_recv,
    yard,
):
    groups, users, routers, heads = sizes
    g = lax.axis_index("groups")
    me = lax.axis_index("users")
    r = lax.axis_index("routers")
    h = lax.axis_index("heads")
    mate = 1 - h
    blocks, width, model = items_v.shape
    slots = x_all.shape[0]
    half_width = q_v.shape[1]
    heads_here = half_width // HEAD_DIM
    hd_all = half_width * heads
    rows = slots * width
    depth = w_all.shape[2]
    out_cols = wo_all.shape[2]
    wh = width // heads
    scale = HEAD_DIM ** (-0.5)
    positions = keys_v.shape[0] * keys_v.shape[1]
    per_user = keys_v.shape[1]

    barrier = pltpu.get_barrier_semaphore()
    count = 0
    for j in range(1, routers):
        pl.semaphore_signal(
            barrier, inc=1, device_id={"routers": lax.rem(r + j, routers)}, device_id_type=MESH
        )
        count += 1
    for i in range(1, groups):
        pl.semaphore_signal(
            barrier, inc=1, device_id={"groups": lax.rem(g + i, groups)}, device_id_type=MESH
        )
        count += 1
    pl.semaphore_signal(barrier, inc=1, device_id={"heads": mate}, device_id_type=MESH)
    count += 1
    for k in range(1, users):
        for e in range(heads):
            pl.semaphore_signal(
                barrier,
                inc=1,
                device_id={"users": lax.rem(me + k, users), "heads": e},
                device_id_type=MESH,
            )
            count += 1
    first = [
        pltpu.make_async_copy(src, dst, local_sem.at[n])
        for n, (src, dst) in enumerate(
            (
                (owner_hbm, owner_ref),
                (user_hbm, user_ref),
                (fill_hbm, fill_ref),
                (items_ref, items_v),
            )
        )
    ]
    gains = [
        pltpu.make_async_copy(src, dst, local_sem.at[4 + n])
        for n, (src, dst) in enumerate(
            (
                (attn_gain_hbm, attn_gain_ref),
                (mlp_gain_hbm, mlp_gain_ref),
                (w_two_hbm, w_two_ref),
            )
        )
    ]
    ahead = PIECES[0][0], PIECES[1][0]
    lead = [
        pltpu.make_async_copy(w_in_ref.at[p], w_all.at[p, r], local_sem.at[8 + n])
        for n, p in enumerate(ahead)
    ]
    later = [p for p in range(4) if p not in ahead]
    bulk = [
        pltpu.make_async_copy(src, dst, local_sem.at[7])
        for src, dst in [(w_in_ref.at[p], w_all.at[p, r]) for p in later]
        + [(w_o_ref, wo_all.at[r])]
    ]
    rest = [
        pltpu.make_async_copy(src, dst, local_sem.at[10])
        for src, dst in ((keys_ref, keys_v), (values_ref, values_v), (w_one_ref, w_one_v))
    ]

    def size(*refs):
        return sum(math.prod(ref.shape) * jnp.dtype(ref.dtype).itemsize for ref in refs)

    def drain(sem, amount):
        part = yard.at[pl.ds(0, amount // (yard.shape[1] * 2)), :]
        pltpu.make_async_copy(part, part, sem).wait()

    for c in lead + first + bulk:
        c.start()
    pl.semaphore_wait(barrier, count)

    pieces = plan(groups, depth, half_width)
    live = [t for t in range(len(pieces)) if pieces[t][3]]
    slot_x = {t: n for n, t in enumerate(live)}
    slot_y = {t: n + 5 for n, t in enumerate(t for t in live if pieces[t][1] == "t")}
    slot_y.update({t: pieces[t][0] for t in live if pieces[t][1] == "g"})
    parity = lax.rem(me, 2)
    pair = me + 1 - 2 * parity

    def weight_slot(owner_router, owner_group, owner_parity, t):
        p, kind, start, length = pieces[t]
        index = {
            "t": owner_group * 2 + owner_parity,
            "g": owner_group,
            "p": owner_parity,
            "o": 0,
        }[kind]
        start = start + index * length
        if kind != "o":
            start = pl.multiple_of(start, 16)
        span = pl.ds(start, length)
        if p < 4:
            return w_all.at[p, owner_router, span, :]
        return wo_all.at[owner_router, span, :]

    def piece_bytes(t):
        return size(weight_slot(0, 0, 0, t))

    def x_copy(j, t, source_router):
        spot = weight_slot(source_router, g, parity, t)
        return pltpu.make_async_remote_copy(
            src_ref=spot,
            dst_ref=spot,
            send_sem=sent.at[0],
            recv_sem=x_recv.at[j - 1, slot_x[t]],
            device_id={"routers": lax.rem(r + j, routers)},
            device_id_type=MESH,
        )

    def y_copy(i, j, t, owner_group):
        spot = weight_slot(lax.rem(r - j + routers, routers), owner_group, parity, t)
        return pltpu.make_async_remote_copy(
            src_ref=spot,
            dst_ref=spot,
            send_sem=sent.at[0],
            recv_sem=y_recv.at[i - 1, j - 1, slot_y[t]],
            device_id={"groups": lax.rem(g + i, groups)},
            device_id_type=MESH,
        )

    def pair_copy(i, j, t):
        spot = weight_slot(
            lax.rem(r - j + routers, routers), lax.rem(g - i + groups, groups), parity, t
        )
        return pltpu.make_async_remote_copy(
            src_ref=spot,
            dst_ref=spot,
            send_sem=sent.at[0],
            recv_sem=w_recv.at[j - 1, pieces[t][0]],
            device_id={"users": pair},
            device_id_type=MESH,
        )

    for n, p in enumerate(ahead):
        lead[n].wait()
        for t in (0, 1):
            if PIECES[t][0] == p and t in live:
                for j in range(1, routers):
                    x_copy(j, t, r).start()
    for c in first[:3]:
        c.wait()
    owners = [owner_ref[b] for b in range(blocks)]
    ranks = []
    for b in range(blocks):
        rank = jnp.int32(0)
        for a in range(b):
            rank = rank + jnp.where(owners[a] == owners[b], 1, 0)
        ranks.append(rank)

    def slot_source(dest, cap):
        index, user = jnp.int32(0), jnp.int32(-1)
        for b in range(blocks):
            hit = (owners[b] == dest) & (ranks[b] == cap)
            index = jnp.where(hit, b, index)
            user = jnp.where(hit, user_ref[b], user)
        return index, user

    mask_bytes = size(mask_out) // users
    slot_bytes = size(out_slots) // users
    cached = keys_v.shape[0]
    row_user = lax.broadcasted_iota(jnp.int32, (8, HEAD_DIM), 0)
    mask_copies, item_copies = {}, {}

    def across(k):
        other = me
        bit = 1
        while bit < users:
            if k & bit:
                other = other + bit - 2 * bit * lax.rem(me // bit, 2)
            bit *= 2
        return other

    def z_copy(k, source):
        return pltpu.make_async_remote_copy(
            src_ref=out_slots.at[k],
            dst_ref=x_all.at[pl.ds(source * CAP, CAP), pl.ds(pl.multiple_of(h * wh, wh), wh), :],
            send_sem=sent.at[0],
            recv_sem=z_recv.at[k - 1],
            device_id={"users": across(k)},
            device_id_type=MESH,
        )

    def m_copy(k, source):
        return pltpu.make_async_remote_copy(
            src_ref=mask_out.at[k],
            dst_ref=mask_all.at[source],
            send_sem=sent.at[0],
            recv_sem=group_recv.at[0],
            device_id={"users": across(k)},
            device_id_type=MESH,
        )

    def relay_copy(k, part):
        spot = x_all.at[
            pl.ds(across(k) * CAP, CAP), pl.ds(pl.multiple_of(part * wh, wh), wh), :
        ]
        return pltpu.make_async_remote_copy(
            src_ref=spot,
            dst_ref=spot,
            send_sem=sent.at[0],
            recv_sem=group_recv.at[2 if k == 1 else 1],
            device_id={"heads": mate},
            device_id_type=MESH,
        )

    for k in list(range(1, users)) + [0]:
        lines = jnp.zeros((8, HEAD_DIM), F32)
        for cap in range(CAP):
            user = slot_source(across(k), cap)[1]
            lines = lines + jnp.where(row_user == user + cap * cached, jnp.where(user < 0, 0.0, 1.0), 0.0)
        if k:
            mask_out[k] = lines
            m_copy(k, me).start()
        else:
            mask_all[me] = lines
    first[3].wait()
    for k in list(range(1, users)) + [0]:
        for cap in range(CAP):
            index = slot_source(across(k), cap)[0]
            if k:
                out_slots[k, cap] = items_v[index, pl.ds(pl.multiple_of(h * wh, wh), wh), :]
            else:
                x_all[me * CAP + cap] = items_v[index]
        if k:
            z_copy(k, me).start()
    drain(local_sem.at[7], size(w_o_ref) + len(later) * (size(w_in_ref) // 4))
    for t in live:
        if t > 1:
            for j in range(1, routers):
                x_copy(j, t, r).start()
    for c in rest + gains:
        c.start()

    def forward(t):
        if t not in live:
            return
        kind = pieces[t][1]
        for j in range(1, routers):
            x_copy(j, t, lax.rem(r - j + routers, routers)).wait_recv()
            if kind in "tg":
                for i in range(1, groups):
                    y_copy(i, j, t, g).start()
            if kind in "tp":
                pair_copy(0, j, t).start()

    def second(t):
        if t not in live:
            return
        for j in range(1, routers):
            for i in range(1, groups):
                y_copy(i, j, t, lax.rem(g - i + groups, groups)).wait_recv()
                pair_copy(i, j, t).start()

    def landed(p):
        mine_of = [t for t in live if pieces[t][0] == p]
        straight = sum(piece_bytes(t) for t in mine_of if pieces[t][1] == "g")
        paired = sum(
            piece_bytes(t) * (groups if pieces[t][1] == "t" else 1)
            for t in mine_of
            if pieces[t][1] in "tp"
        )
        for j in range(1, routers):
            for t in mine_of:
                if pieces[t][1] == "o":
                    x_copy(j, t, lax.rem(r - j + routers, routers)).wait_recv()
            for i in range(1, groups):
                if straight:
                    drain(y_recv.at[i - 1, j - 1, p], straight)
            if paired:
                drain(w_recv.at[j - 1, p], paired)

    tile_slots = 4
    tile = tile_slots * width
    tiles = rows // tile

    def x_tile(i):
        return x_all[pl.ds(i * tile_slots, tile_slots)].reshape(tile, model)

    def span_of(i):
        return pl.ds(pl.multiple_of(i * tile, tile), tile)

    def projected(p, i):
        x = x_tile(i)
        total = jnp.zeros((tile, half_width), F32)
        for a in range(routers):
            total = total + jnp.dot(
                x[:, a * depth : (a + 1) * depth], w_all[p, a], preferred_element_type=F32
            )
        return silu(total)

    def query(i):
        q_v[span_of(i), :] = projected(0, i).astype(BF16)

    def turn():
        gain_v[...] = mlp_gain_ref[...].astype(F32).reshape(1, -1)
        for e in range(heads_here):
            for u in range(cached):
                turned[e, u * HEAD_DIM : (u + 1) * HEAD_DIM, :] = keys_v[
                    u, :, e * HEAD_DIM : (e + 1) * HEAD_DIM
                ].T

    def attend(i, part):
        span = span_of(i)
        picks = []
        for u in range(cached):
            lines = []
            for s in range(tile_slots):
                spot = s % CAP * cached + u
                line = mask_all[i * (tile_slots // CAP) + s // CAP, spot : spot + 1, :]
                lines.append(jnp.broadcast_to(line, (width, HEAD_DIM)))
            picks.append(jnp.concatenate(lines, axis=0).astype(BF16))
        share = heads_here // 2
        for e in range(part * share, (part + 1) * share):
            cols = slice(e * HEAD_DIM, (e + 1) * HEAD_DIM)
            q = q_v[span, cols]
            raw = jnp.dot(
                jnp.concatenate([q * pick for pick in picks], axis=1),
                turned[e],
                preferred_element_type=F32,
            )
            weights = silu(raw * scale).astype(BF16)
            wide = per_user // HEAD_DIM
            weights = jnp.concatenate(
                [weights * jnp.concatenate([pick] * wide, axis=1) for pick in picks], axis=1
            )
            att_v[span, cols] = (
                jnp.dot(
                    weights,
                    values_v[:, :, cols].reshape(positions, HEAD_DIM),
                    preferred_element_type=F32,
                )
                .astype(BF16)
                .astype(F32)
            )

    def self_key(i):
        span = span_of(i)
        keys = projected(1, i)
        for e in range(heads_here):
            cols = slice(e * HEAD_DIM, (e + 1) * HEAD_DIM)
            own = jnp.sum(q_v[span, cols].astype(F32) * keys[:, cols], axis=1, keepdims=True)
            own_v[span, cols] = jnp.broadcast_to(silu(own * scale), (tile, HEAD_DIM))

    lane = lax.broadcasted_iota(jnp.int32, (tile, 128), 1)

    def self_value(i):
        span = span_of(i)
        att = att_v[span, :] + own_v[span, :] * projected(2, i)
        att_v[span, :] = att
        total = jnp.sum(att, axis=1, keepdims=True)
        square = jnp.sum(att * att, axis=1, keepdims=True)
        stat_out[span, :] = jnp.where(lane == 0, total, square)

    def gate(i):
        span = span_of(i)
        both = stat_out[span, :] + stat_in[span, :]
        mean = both[:, 0:1] / hd_all
        var = both[:, 1:2] / hd_all - mean * mean
        gated_v[span, :] = (
            (att_v[span, :] - mean)
            * lax.rsqrt(var + EPSILON)
            * attn_gain_ref[...].astype(F32).reshape(1, -1)
            * projected(3, i)
        ).astype(BF16)

    def stat_copy(i):
        return pltpu.make_async_remote_copy(
            src_ref=stat_out.at[span_of(i), :],
            dst_ref=stat_in.at[span_of(i), :],
            send_sem=sent.at[0],
            recv_sem=st_recv.at[i],
            device_id={"heads": mate},
            device_id_type=MESH,
        )

    near = me // (tile_slots // CAP)

    def over(fun, which, *args):
        if which == "A":
            fun(near, *args)
        elif tiles == 2:
            fun(1 - near, *args)
        else:

            @pl.loop(1, tiles)
            def _(n):
                fun(lax.rem(near + n, tiles), *args)

    def value(i):
        self_value(i)
        stat_copy(i).start()

    def gating(i):
        stat_copy(i).wait_recv()
        gate(i)

    def halves(fun, which):
        share = tiles // 2
        for i in range(which * share, (which + 1) * share):
            fun(i)

    half = rows // heads

    mine = users // heads
    seat, seat_mate = heads - 1 - h, heads - 1 - mate
    piece = half // 2
    source_rows = CAP * width

    def far_first(e, i, amount):
        return jnp.where(me < e * mine + mine // 2, amount - 1 - i, i)

    def part_copy(j, c):
        spot = pl.ds(pl.multiple_of(c * piece, piece), piece)
        return pltpu.make_async_remote_copy(
            src_ref=part_out.at[j, spot, :],
            dst_ref=part_in.at[j, spot, :],
            send_sem=sent.at[0],
            recv_sem=po_recv.at[c if j == 0 else 2 + c],
            device_id={"heads": mate},
            device_id_type=MESH,
        )

    def out_project(j, row_half, c, target):
        src = pl.ds(pl.multiple_of(row_half * half + c * piece, piece), piece)
        target[j, pl.ds(pl.multiple_of(c * piece, piece), piece), :] = jnp.dot(
            gated_v[src, :],
            wo_all[lax.rem(r - j + routers, routers)],
            preferred_element_type=F32,
        ).astype(target.dtype)

    def shares(j):
        for i in range(2):
            c = far_first(seat_mate, i, 2)
            out_project(j, seat_mate, c, part_out)
            part_copy(j, c).start()

    def outer(js):
        for j in js:
            shares(j)
        for j in js:
            part_own[j] = jnp.dot(
                gated_v[pl.ds(pl.multiple_of(seat * half, half), half), :],
                wo_all[lax.rem(r - j + routers, routers)],
                preferred_element_type=F32,
            )

    def step(name):
        if name == "T":
            drain(local_sem.at[10], size(keys_ref, values_ref, w_one_ref))
            for c in gains:
                c.wait()
            turn()
        elif name[0] == "f":
            forward(int(name[1:]))
        elif name[0] == "z":
            second(int(name[1:]))
        elif name[0] == "L":
            landed(int(name[1:]))
        elif name[0] == "r" and name[1] in "AB":
            if name[1] == "A":
                drain(group_recv.at[2], slot_bytes)
                drain(group_recv.at[0], (users - 1) * mask_bytes)
            else:
                drain(group_recv.at[1], (users - 2) * slot_bytes)
        elif name[0] == "r":
            for k in range(int(name[1:]), users if name == "r3" else int(name[1:]) + 1):
                z_copy(k, across(k)).wait_recv()
                relay_copy(k, h).start()
        elif name[0] == "q":
            over(query, name[1])
        elif name[0] == "a":
            over(attend, name[1], int(name[2]))
        elif name[0] == "k":
            over(self_key, name[1])
        elif name[0] == "v":
            halves(value, int(name[1]))
        elif name[0] == "g":
            halves(gating, int(name[1]))
        elif name == "o0":
            outer([0])
        else:
            outer(range(1, routers))

    for name in STEPS:
        with jax.named_scope(name):
            step(name)

    two = jnp.broadcast_to(
        w_two_ref[...].astype(F32).reshape(1, -1), (8, w_two_ref.shape[0])
    ).astype(BF16)

    def mixed(source, j):
        a = lax.rem(r - j + routers, routers)
        span = pl.ds(pl.multiple_of(source * source_rows, source_rows), source_rows)
        cols = pl.ds(pl.multiple_of(a * out_cols, out_cols), out_cols)
        x = x_all[pl.ds((seat * mine + source) * CAP, CAP), :, cols]
        x = x.reshape(source_rows, out_cols).astype(F32)
        residual = x + part_own[j, span, :] + part_in[j, span, :].astype(F32)
        square = jnp.sum(residual * residual, axis=1, keepdims=True)
        scaled = (residual * gain_v[:, cols]).astype(BF16)
        return square, jnp.dot(scaled, w_one_v[cols, :], preferred_element_type=F32)

    def score(source, i, square, total):
        for j in range(1, routers):
            more = mixed(source, j)
            square, total = square + more[0], total + more[1]
        norm = lax.rsqrt(square / model + EPSILON)
        hidden = silu(norm * total).astype(BF16)
        sc_out[i] = lax.dot_general(
            two, hidden, (((1,), (1,)), ((), ())), preferred_element_type=F32
        )

    def score_copy(i, e, owner, sem):
        return pltpu.make_async_remote_copy(
            src_ref=sc_out.at[i],
            dst_ref=ret.at[owner],
            send_sem=sc_send.at[i, e],
            recv_sem=sc_recv.at[sem],
            device_id={"users": seat * mine + far_first(seat, i, mine), "heads": e},
            device_id_type=MESH,
        )

    group = mine // 2
    early = {}
    with jax.named_scope("early"):
        for i in range(mine):
            source = far_first(seat, i, mine)
            if i % group == 0:
                drain(po_recv.at[far_first(seat, i // group, 2)], piece * out_cols * 2)
            early[i] = mixed(source, 0)
    for i in range(mine):
        source = far_first(seat, i, mine)
        if i % group == 0:
            with jax.named_scope("partwait"):
                drain(
                    po_recv.at[2 + far_first(seat, i // group, 2)],
                    (routers - 1) * piece * out_cols * 2,
                )
        with jax.named_scope("score"):
            score(source, i, *early[i])
        target = seat * mine + source
        for e in range(heads):
            itself = (target == me) & (h == e)

            @pl.when(jnp.logical_not(itself))
            def _():
                score_copy(i, e, me, me).start()

            @pl.when(itself)
            def _():
                ret[me] = sc_out[i]

    rounds = {"t": 1 + (groups - 1) + groups, "g": groups, "p": 2, "o": 1}
    hops = sum(piece_bytes(t) * rounds[pieces[t][1]] for t in live)
    total = (routers - 1) * hops + (users - 1) * (2 * slot_bytes + mask_bytes)
    drain(sent.at[0], total + size(stat_out) + size(part_out))
    handler = heads - 1 - me // mine
    with jax.named_scope("scorewait"):
        for d in range(users):

            @pl.when(jnp.logical_not((d == me) & (h == handler)))
            def _():
                score_copy(0, 0, d, d).wait_recv()

    position = lax.broadcasted_iota(jnp.int32, (1, width), 1)
    for b in range(blocks):
        tile_in = ret[owners[b]]
        line = tile_in[0:1, 0:width]
        for cap in range(1, CAP):
            line = jnp.where(ranks[b] == cap, tile_in[0:1, cap * width : (cap + 1) * width], line)
        out_ref[b : b + 1, :] = jnp.where(position < fill_ref[b], line, 0.0)

    for i in range(mine):
        for e in range(heads):

            @pl.when(jnp.logical_not((seat * mine + far_first(seat, i, mine) == me) & (h == e)))
            def _():
                score_copy(i, e, me, me).wait_send()


def local(
    sizes,
    items,
    block_owner,
    block_user,
    block_fill,
    prefix_keys,
    prefix_values,
    w_in,
    attn_gain,
    w_o,
    mlp_gain,
    w_one,
    w_two,
):
    groups, users, routers, heads = sizes
    blocks, width, model = items.shape
    projections, depth, half_width = w_in.shape
    slots = users * CAP
    rows = slots * width
    half = rows // heads
    out_cols = w_o.shape[1]
    cached, per_user, _ = prefix_keys.shape
    positions = cached * per_user
    pieces = plan(groups, depth, half_width)
    live = sum(1 for piece in pieces if piece[3])
    trees = sum(1 for piece in pieces if piece[3] and piece[1] == "t")
    dma = pltpu.SemaphoreType.DMA
    yard_bytes = 2 * (
        (routers - 1) * (w_in.size + w_o.size)
        + (users - 1) * (2 * CAP * (width // heads) * model + 2 * 8 * HEAD_DIM)
        + 2 * 2 * rows * 128
        + routers * half * out_cols
    )
    yard_rows = yard_bytes // 256 // 8 * 8
    hbm = pl.BlockSpec(memory_space=pl.ANY)
    vmem = pl.BlockSpec(memory_space=pltpu.VMEM)
    scratch = [
        pltpu.SMEM((blocks,), jnp.int32),
        pltpu.SMEM((blocks,), jnp.int32),
        pltpu.SMEM((blocks,), jnp.int32),
        pltpu.VMEM(attn_gain.shape, BF16),
        pltpu.VMEM(mlp_gain.shape, BF16),
        pltpu.VMEM(w_two.shape, BF16),
        pltpu.VMEM((blocks, width, model), BF16),
        pltpu.VMEM((users, CAP, width // heads, model), BF16),
        pltpu.VMEM((slots, width, model), BF16),
        pltpu.VMEM((users, 8, HEAD_DIM), F32),
        pltpu.VMEM((users, 8, HEAD_DIM), F32),
        pltpu.VMEM(prefix_keys.shape, BF16),
        pltpu.VMEM(prefix_values.shape, BF16),
        pltpu.VMEM((half_width // HEAD_DIM, cached * HEAD_DIM, per_user), BF16),
        pltpu.VMEM((1, model), F32),
        pltpu.VMEM((projections, routers, depth, half_width), BF16),
        pltpu.VMEM((routers, half_width, out_cols), BF16),
        pltpu.VMEM(w_one.shape, BF16),
        pltpu.VMEM((rows, half_width), BF16),
        pltpu.VMEM((rows, half_width), F32),
        pltpu.VMEM((rows, half_width), F32),
        pltpu.VMEM((rows, half_width), BF16),
        pltpu.VMEM((rows, 128), F32),
        pltpu.VMEM((rows, 128), F32),
        pltpu.VMEM((routers, half, out_cols), BF16),
        pltpu.VMEM((routers, half, out_cols), F32),
        pltpu.VMEM((routers, half, out_cols), BF16),
        pltpu.VMEM((users // heads, 8, CAP * width), F32),
        pltpu.VMEM((users, 8, CAP * width), F32),
        dma((11,)),
        dma((1,)),
        dma((users - 1,)),
        dma((3,)),
        dma((routers - 1, live)),
        dma((groups - 1, routers - 1, 5 + trees)),
        dma((routers - 1, 5)),
        dma((rows // (4 * width),)),
        dma((4,)),
        dma((users // heads, heads)),
        dma((users,)),
        pltpu.VMEM((yard_rows, 128), BF16),
    ]
    return pl.pallas_call(
        functools.partial(scorer, sizes),
        out_shape=pltpu.VMEM((blocks, width), F32),
        in_specs=[hbm] * 12,
        out_specs=vmem,
        scratch_shapes=scratch,
        compiler_params=pltpu.CompilerParams(
            collective_id=0, has_side_effects=True, vmem_limit_bytes=62 * 1024 * 1024
        ),
    )(
        items,
        block_owner.reshape(-1),
        block_user,
        block_fill,
        prefix_keys,
        prefix_values,
        w_in,
        attn_gain,
        w_o,
        mlp_gain,
        w_one,
        w_two,
    )


def solution(mesh):
    placed = (
        P(("groups", "users", "routers"), None, None),
        P(("groups", "users", "routers"), None),
        P(("groups", "users", "routers")),
        P(("groups", "users", "routers")),
        P(("groups", "users"), None, "heads"),
        P(("groups", "users"), None, "heads"),
        P(None, "routers", "heads"),
        P("heads"),
        P("heads", "routers"),
        P(),
        P(),
        P(),
    )
    sizes = tuple(mesh.shape[name] for name in ("groups", "users", "routers", "heads"))
    return jax.shard_map(
        functools.partial(local, sizes),
        mesh=mesh,
        in_specs=placed,
        out_specs=P(("groups", "users", "routers"), None),
        check_vma=False,
    )
```

```python
import functools
import math

import jax
import jax.numpy as jnp
from jax import lax
from jax.experimental import pallas as pl
from jax.experimental.pallas import tpu as pltpu
from jax.sharding import PartitionSpec as P

HEAD_DIM = 128
CAP = 2
EPSILON = 1e-05
UNIT = 512
PIECES = (
    (1, "t", 112),
    (0, "g", 80),
    (2, "t", 80),
    (0, "g", 80),
    (0, "g", 96),
    (3, "t", 64),
    (1, "g", 32),
    (3, "t", 32),
    (2, "g", 96),
    (3, "g", 64),
    (4, "g", 96),
    (4, "p", 32),
    (4, "p", 32),
    (4, "o", 192),
    (3, "o", 0),
    (2, "o", 0),
    (1, "o", 0),
    (0, "o", 0),
)
STEPS = (
    "T", "f0", "f1", "f2", "r1", "r2", "z0", "f3", "f4", "r3", "z2", "f5", "f6", "rA", "rB", "f7",
    "p0", "p1", "p2", "p3", "f8", "L0", "q", "a0", "f9", "z5", "a1", "L1", "k", "z7", "f10", "f11",
    "f12", "L2", "v", "L3", "g0", "g1", "o0", "L4", "o1",
)
F32 = jnp.float32
BF16 = jnp.bfloat16
MESH = pl.DeviceIdType.MESH


def silu(v):
    return 0.5 * v * (1.0 + jnp.tanh(0.5 * v))


def plan(groups, depth, half_width):
    copies = {"t": groups * 2, "g": groups, "p": 2, "o": 1}
    lengths = [depth] * 4 + [half_width]
    filled = [0] * 5
    pieces = []
    for p, kind, share in PIECES:
        count = 0 if kind == "o" else share * lengths[p] // UNIT // 16 * 16
        pieces.append([p, kind, filled[p], count])
        filled[p] += copies[kind] * count
    for n, piece in enumerate(pieces):
        p = piece[0]
        if piece[1] == "o":
            left = lengths[p] - filled[p]
            if any(q[:2] == piece[:2] for q in pieces[n + 1 :]):
                left = min(left, PIECES[n][2] * lengths[p] // UNIT // 16 * 16)
            piece[2:] = filled[p], left
            filled[p] += left
    return pieces


def scorer(
    sizes,
    items_ref,
    owner_hbm,
    user_hbm,
    fill_hbm,
    keys_ref,
    values_ref,
    w_in_ref,
    attn_gain_hbm,
    w_o_ref,
    mlp_gain_hbm,
    w_one_ref,
    w_two_hbm,
    out_ref,
    owner_ref,
    user_ref,
    fill_ref,
    attn_gain_ref,
    mlp_gain_ref,
    w_two_ref,
    items_v,
    out_slots,
    x_all,
    mask_out,
    mask_all,
    keys_v,
    values_v,
    turned,
    gain_v,
    pick_v,
    gate_v,
    pre_v,
    w_all,
    wo_all,
    w_one_v,
    q_v,
    own_v,
    att_v,
    gated_v,
    stat_out,
    stat_in,
    part_out,
    part_own,
    part_in,
    sc_out,
    ret,
    local_sem,
    sent,
    z_recv,
    group_recv,
    x_recv,
    y_recv,
    w_recv,
    st_recv,
    po_recv,
    sc_send,
    sc_recv,
    yard,
):
    groups, users, routers, heads = sizes
    g = lax.axis_index("groups")
    me = lax.axis_index("users")
    r = lax.axis_index("routers")
    h = lax.axis_index("heads")
    mate = 1 - h
    blocks, width, model = items_v.shape
    slots = x_all.shape[0]
    half_width = q_v.shape[1]
    heads_here = half_width // HEAD_DIM
    hd_all = half_width * heads
    rows = slots * width
    depth = w_all.shape[2]
    out_cols = wo_all.shape[2]
    wh = width // heads
    scale = HEAD_DIM ** (-0.5)
    positions = keys_v.shape[0] * keys_v.shape[1]
    per_user = keys_v.shape[1]

    barrier = pltpu.get_barrier_semaphore()
    count = 0
    for j in range(1, routers):
        pl.semaphore_signal(
            barrier, inc=1, device_id={"routers": lax.rem(r + j, routers)}, device_id_type=MESH
        )
        count += 1
    for i in range(1, groups):
        pl.semaphore_signal(
            barrier, inc=1, device_id={"groups": lax.rem(g + i, groups)}, device_id_type=MESH
        )
        count += 1
    pl.semaphore_signal(barrier, inc=1, device_id={"heads": mate}, device_id_type=MESH)
    count += 1
    for k in range(1, users):
        for e in range(heads):
            pl.semaphore_signal(
                barrier,
                inc=1,
                device_id={"users": lax.rem(me + k, users), "heads": e},
                device_id_type=MESH,
            )
            count += 1
    first = [
        pltpu.make_async_copy(src, dst, local_sem.at[n])
        for n, (src, dst) in enumerate(
            (
                (owner_hbm, owner_ref),
                (user_hbm, user_ref),
                (fill_hbm, fill_ref),
                (items_ref, items_v),
            )
        )
    ]
    gains = [
        pltpu.make_async_copy(src, dst, local_sem.at[4 + n])
        for n, (src, dst) in enumerate(
            (
                (attn_gain_hbm, attn_gain_ref),
                (mlp_gain_hbm, mlp_gain_ref),
                (w_two_hbm, w_two_ref),
            )
        )
    ]
    order = [p for p, _, _ in PIECES]
    ahead = list(dict.fromkeys(order))[:2]
    opening = min(t for t, p in enumerate(order) if p not in ahead)
    lead = [
        pltpu.make_async_copy(w_in_ref.at[p], w_all.at[p, r], local_sem.at[8 + n])
        for n, p in enumerate(ahead)
    ]
    later = [p for p in range(4) if p not in ahead]
    bulk = [
        pltpu.make_async_copy(src, dst, local_sem.at[7])
        for src, dst in [(w_in_ref.at[p], w_all.at[p, r]) for p in later]
        + [(w_o_ref, wo_all.at[r])]
    ]
    rest = [
        pltpu.make_async_copy(src, dst, local_sem.at[10])
        for src, dst in ((keys_ref, keys_v), (values_ref, values_v), (w_one_ref, w_one_v))
    ]

    def size(*refs):
        return sum(math.prod(ref.shape) * jnp.dtype(ref.dtype).itemsize for ref in refs)

    def drain(sem, amount):
        part = yard.at[pl.ds(0, amount // (yard.shape[1] * 2)), :]
        pltpu.make_async_copy(part, part, sem).wait()

    for c in lead + first + bulk:
        c.start()
    pl.semaphore_wait(barrier, count)

    pieces = plan(groups, depth, half_width)
    live = [t for t in range(len(pieces)) if pieces[t][3]]
    slot_x = {t: n for n, t in enumerate(live)}
    slot_y = {t: n + 5 for n, t in enumerate(t for t in live if pieces[t][1] == "t")}
    slot_y.update({t: pieces[t][0] for t in live if pieces[t][1] == "g"})
    parity = lax.rem(me, 2)
    pair = me + 1 - 2 * parity

    def weight_slot(owner_router, owner_group, owner_parity, t):
        p, kind, start, length = pieces[t]
        index = {
            "t": owner_group * 2 + owner_parity,
            "g": owner_group,
            "p": owner_parity,
            "o": 0,
        }[kind]
        start = start + index * length
        if kind != "o":
            start = pl.multiple_of(start, 16)
        span = pl.ds(start, length)
        if p < 4:
            return w_all.at[p, owner_router, span, :]
        return wo_all.at[owner_router, span, :]

    def piece_bytes(t):
        return size(weight_slot(0, 0, 0, t))

    def x_copy(j, t, source_router):
        spot = weight_slot(source_router, g, parity, t)
        return pltpu.make_async_remote_copy(
            src_ref=spot,
            dst_ref=spot,
            send_sem=sent.at[0],
            recv_sem=x_recv.at[j - 1, slot_x[t]],
            device_id={"routers": lax.rem(r + j, routers)},
            device_id_type=MESH,
        )

    def y_copy(i, j, t, owner_group):
        spot = weight_slot(lax.rem(r - j + routers, routers), owner_group, parity, t)
        return pltpu.make_async_remote_copy(
            src_ref=spot,
            dst_ref=spot,
            send_sem=sent.at[0],
            recv_sem=y_recv.at[i - 1, j - 1, slot_y[t]],
            device_id={"groups": lax.rem(g + i, groups)},
            device_id_type=MESH,
        )

    def pair_copy(i, j, t):
        spot = weight_slot(
            lax.rem(r - j + routers, routers), lax.rem(g - i + groups, groups), parity, t
        )
        return pltpu.make_async_remote_copy(
            src_ref=spot,
            dst_ref=spot,
            send_sem=sent.at[0],
            recv_sem=w_recv.at[j - 1, pieces[t][0]],
            device_id={"users": pair},
            device_id_type=MESH,
        )

    def send_x(t):
        if t in live:
            for j in range(1, routers):
                x_copy(j, t, r).start()

    def send_first():
        lead[0].wait()
        for t in range(opening):
            if order[t] != ahead[0] and ahead[1] not in order[:t]:
                lead[1].wait()
            send_x(t)

    send_first()
    for c in first[:3]:
        c.wait()
    owners = [owner_ref[b] for b in range(blocks)]
    ranks = []
    for b in range(blocks):
        rank = jnp.int32(0)
        for a in range(b):
            rank = rank + jnp.where(owners[a] == owners[b], 1, 0)
        ranks.append(rank)

    def slot_source(dest, cap):
        index, user = jnp.int32(0), jnp.int32(-1)
        for b in range(blocks):
            hit = (owners[b] == dest) & (ranks[b] == cap)
            index = jnp.where(hit, b, index)
            user = jnp.where(hit, user_ref[b], user)
        return index, user

    mask_bytes = size(mask_out) // users
    slot_bytes = size(out_slots) // users
    cached = keys_v.shape[0]
    row_user = lax.broadcasted_iota(jnp.int32, (8, HEAD_DIM), 0)
    mask_copies, item_copies = {}, {}

    def across(k):
        other = me
        bit = 1
        while bit < users:
            if k & bit:
                other = other + bit - 2 * bit * lax.rem(me // bit, 2)
            bit *= 2
        return other

    def z_copy(k, source):
        return pltpu.make_async_remote_copy(
            src_ref=out_slots.at[k],
            dst_ref=x_all.at[pl.ds(source * CAP, CAP), pl.ds(pl.multiple_of(h * wh, wh), wh), :],
            send_sem=sent.at[0],
            recv_sem=z_recv.at[k - 1],
            device_id={"users": across(k)},
            device_id_type=MESH,
        )

    def m_copy(k, source):
        return pltpu.make_async_remote_copy(
            src_ref=mask_out.at[k],
            dst_ref=mask_all.at[source],
            send_sem=sent.at[0],
            recv_sem=group_recv.at[0],
            device_id={"users": across(k)},
            device_id_type=MESH,
        )

    def relay_copy(k, part):
        spot = x_all.at[
            pl.ds(across(k) * CAP, CAP), pl.ds(pl.multiple_of(part * wh, wh), wh), :
        ]
        return pltpu.make_async_remote_copy(
            src_ref=spot,
            dst_ref=spot,
            send_sem=sent.at[0],
            recv_sem=group_recv.at[2 if k == 1 else 1],
            device_id={"heads": mate},
            device_id_type=MESH,
        )

    for k in list(range(1, users)) + [0]:
        lines = jnp.zeros((8, HEAD_DIM), F32)
        for cap in range(CAP):
            user = slot_source(across(k), cap)[1]
            lines = lines + jnp.where(row_user == user + cap * cached, jnp.where(user < 0, 0.0, 1.0), 0.0)
        if k:
            mask_out[k] = lines
            m_copy(k, me).start()
        else:
            mask_all[me] = lines
    first[3].wait()
    for k in list(range(1, users)) + [0]:
        for cap in range(CAP):
            index = slot_source(across(k), cap)[0]
            if k:
                out_slots[k, cap] = items_v[index, pl.ds(pl.multiple_of(h * wh, wh), wh), :]
            else:
                x_all[me * CAP + cap] = items_v[index]
        if k:
            z_copy(k, me).start()
    drain(local_sem.at[7], size(w_o_ref) + len(later) * (size(w_in_ref) // 4))
    for t in range(opening, len(pieces)):
        send_x(t)
    for c in rest + gains:
        c.start()

    def forward(t):
        if t not in live:
            return
        kind = pieces[t][1]
        for j in range(1, routers):
            x_copy(j, t, lax.rem(r - j + routers, routers)).wait_recv()
            if kind in "tg":
                for i in range(1, groups):
                    y_copy(i, j, t, g).start()
            if kind in "tp":
                pair_copy(0, j, t).start()

    def second(t):
        if t not in live:
            return
        for j in range(1, routers):
            for i in range(1, groups):
                y_copy(i, j, t, lax.rem(g - i + groups, groups)).wait_recv()
                pair_copy(i, j, t).start()

    def landed(p):
        mine_of = [t for t in live if pieces[t][0] == p]
        straight = sum(piece_bytes(t) for t in mine_of if pieces[t][1] == "g")
        paired = sum(
            piece_bytes(t) * (groups if pieces[t][1] == "t" else 1)
            for t in mine_of
            if pieces[t][1] in "tp"
        )
        for j in range(1, routers):
            for t in mine_of:
                if pieces[t][1] == "o":
                    x_copy(j, t, lax.rem(r - j + routers, routers)).wait_recv()
            for i in range(1, groups):
                if straight:
                    drain(y_recv.at[i - 1, j - 1, p], straight)
            if paired:
                drain(w_recv.at[j - 1, p], paired)

    tile_slots = 4
    tile = tile_slots * width

    wide = 2 * tile

    def wide_span(i):
        return pl.ds(pl.multiple_of(i * wide, wide), wide)

    def product(p, i, a):
        cols = pl.ds(pl.multiple_of(a * depth, depth), depth)
        x = x_all[pl.ds(i * 2 * tile_slots, 2 * tile_slots), :, cols]
        return jnp.dot(x.reshape(wide, depth), w_all[p, a], preferred_element_type=F32)

    def prepare(i, p):
        pre_v[p, wide_span(i), :] = product(p, i, r)

    def projected(p, i):
        total = pre_v[p, wide_span(i), :]
        for j in range(1, routers):
            total = total + product(p, i, lax.rem(r - j + routers, routers))
        return silu(total)

    def query(i):
        q_v[wide_span(i), :] = projected(0, i).astype(BF16)

    def turn():
        gain_v[...] = mlp_gain_ref[...].astype(F32).reshape(1, -1)
        for e in range(heads_here):
            for u in range(cached):
                turned[e, u * HEAD_DIM : (u + 1) * HEAD_DIM, :] = keys_v[
                    u, :, e * HEAD_DIM : (e + 1) * HEAD_DIM
                ].T

    def picking(i):
        for s in range(2 * tile_slots):
            for u in range(cached):
                spot = s % CAP * cached + u
                line = mask_all[i * (2 * tile_slots // CAP) + s // CAP, spot : spot + 1, :]
                rows_s = pl.ds(pl.multiple_of(i * wide + s * width, width), width)
                pick_v[u, rows_s, :] = jnp.broadcast_to(line, (width, HEAD_DIM)).astype(BF16)

    def attend(i, part):
        span = wide_span(i)
        picks = [pick_v[u, span, :] for u in range(cached)]
        share = heads_here // 2
        for e in range(part * share, (part + 1) * share):
            cols = slice(e * HEAD_DIM, (e + 1) * HEAD_DIM)
            q = q_v[span, cols]
            raw = jnp.dot(
                jnp.concatenate([q * pick for pick in picks], axis=1),
                turned[e],
                preferred_element_type=F32,
            )
            weights = silu(raw * scale).astype(BF16)
            times = per_user // HEAD_DIM
            weights = jnp.concatenate(
                [weights * jnp.concatenate([pick] * times, axis=1) for pick in picks], axis=1
            )
            att_v[span, cols] = (
                jnp.dot(
                    weights,
                    values_v[:, :, cols].reshape(positions, HEAD_DIM),
                    preferred_element_type=F32,
                )
                .astype(BF16)
                .astype(F32)
            )

    def self_key(i):
        span = wide_span(i)
        keys = projected(1, i)
        for e in range(heads_here):
            cols = slice(e * HEAD_DIM, (e + 1) * HEAD_DIM)
            own = jnp.sum(q_v[span, cols].astype(F32) * keys[:, cols], axis=1, keepdims=True)
            own_v[span, cols] = jnp.broadcast_to(silu(own * scale), (wide, HEAD_DIM))

    lane = lax.broadcasted_iota(jnp.int32, (width, 128), 1)

    def self_value(i):
        span = wide_span(i)
        att = att_v[span, :] + own_v[span, :] * projected(2, i)
        att_v[span, :] = att
        total = jnp.sum(att, axis=1, keepdims=True)
        square = jnp.sum(att * att, axis=1, keepdims=True)
        packed = jnp.zeros((width, 128), F32)
        for b in range(wide // width):
            part = slice(b * width, (b + 1) * width)
            packed = jnp.where(lane == 2 * b, total[part], packed)
            packed = jnp.where(lane == 2 * b + 1, square[part], packed)
        stat_out[i] = packed

    def gate(i):
        gate_v[wide_span(i), :] = attn_gain_ref[...].astype(F32).reshape(1, -1) * projected(3, i)

    def gating(i):
        stat_copy(i).wait_recv()
        both = stat_out[i] + stat_in[i]
        for b in range(wide // width):
            span = pl.ds(pl.multiple_of(i * wide + b * width, width), width)
            mean = both[:, 2 * b : 2 * b + 1] / hd_all
            var = both[:, 2 * b + 1 : 2 * b + 2] / hd_all - mean * mean
            gated_v[span, :] = (
                (att_v[span, :] - mean) * lax.rsqrt(var + EPSILON) * gate_v[span, :]
            ).astype(BF16)

    def stat_copy(i):
        return pltpu.make_async_remote_copy(
            src_ref=stat_out.at[i],
            dst_ref=stat_in.at[i],
            send_sem=sent.at[0],
            recv_sem=st_recv.at[i],
            device_id={"heads": mate},
            device_id_type=MESH,
        )

    def value(i):
        self_value(i)
        stat_copy(i).start()

    def whole(fun):
        for i in range(rows // wide):
            fun(i)

    half = rows // heads

    mine = users // heads
    seat, seat_mate = heads - 1 - h, heads - 1 - mate
    piece = half // 2
    source_rows = CAP * width

    def far_first(e, i, amount):
        return jnp.where(me < e * mine + mine // 2, amount - 1 - i, i)

    def part_copy(j, c):
        spot = pl.ds(pl.multiple_of(c * piece, piece), piece)
        return pltpu.make_async_remote_copy(
            src_ref=part_out.at[j, spot, :],
            dst_ref=part_in.at[j, spot, :],
            send_sem=sent.at[0],
            recv_sem=po_recv.at[c if j == 0 else 2 + c],
            device_id={"heads": mate},
            device_id_type=MESH,
        )

    def shares(j):
        pieces_of = (half,) if j == 0 else (piece, piece)
        for i, count in enumerate(pieces_of):
            c = 0 if j == 0 else far_first(seat_mate, i, 2)
            start = pl.multiple_of(c * piece, piece)
            part_out[j, pl.ds(start, count), :] = jnp.dot(
                gated_v[pl.ds(pl.multiple_of(seat_mate * half + start, piece), count), :],
                wo_all[lax.rem(r - j + routers, routers)],
                preferred_element_type=F32,
            ).astype(BF16)
            if j:
                part_copy(j, c).start()
        if j == 0:
            for i in range(2):
                part_copy(j, far_first(seat_mate, i, 2)).start()

    def outer(js):
        for j in js:
            shares(j)
        for j in js:
            part_own[j] = jnp.dot(
                gated_v[pl.ds(pl.multiple_of(seat * half, half), half), :],
                wo_all[lax.rem(r - j + routers, routers)],
                preferred_element_type=F32,
            )

    def step(name):
        if name == "T":
            drain(local_sem.at[10], size(keys_ref, values_ref, w_one_ref))
            for c in gains:
                c.wait()
            turn()
        elif name[0] == "f":
            forward(int(name[1:]))
        elif name[0] == "z":
            second(int(name[1:]))
        elif name[0] == "L":
            landed(int(name[1:]))
        elif name[0] == "r" and name[1] in "AB":
            if name[1] == "A":
                drain(group_recv.at[2], slot_bytes)
                drain(group_recv.at[0], (users - 1) * mask_bytes)
                whole(picking)
            else:
                drain(group_recv.at[1], (users - 2) * slot_bytes)
        elif name[0] == "r":
            for k in range(int(name[1:]), users if name == "r3" else int(name[1:]) + 1):
                z_copy(k, across(k)).wait_recv()
                relay_copy(k, h).start()
        elif name[0] == "p":
            whole(functools.partial(prepare, p=int(name[1])))
        elif name[0] == "q":
            whole(query)
        elif name[0] == "a":
            whole(functools.partial(attend, part=int(name[1])))
        elif name[0] == "k":
            whole(self_key)
        elif name[0] == "v":
            whole(value)
        elif name == "g0":
            whole(gate)
        elif name == "g1":
            whole(gating)
        elif name == "o0":
            outer([0])
        else:
            outer(range(1, routers))

    for name in STEPS:
        with jax.named_scope(name):
            step(name)

    two = jnp.broadcast_to(
        w_two_ref[...].astype(F32).reshape(1, -1), (8, w_two_ref.shape[0])
    ).astype(BF16)

    def mixed(source, j):
        a = lax.rem(r - j + routers, routers)
        span = pl.ds(pl.multiple_of(source * source_rows, source_rows), source_rows)
        cols = pl.ds(pl.multiple_of(a * out_cols, out_cols), out_cols)
        x = x_all[pl.ds((seat * mine + source) * CAP, CAP), :, cols]
        x = x.reshape(source_rows, out_cols).astype(F32)
        residual = x + part_own[j, span, :] + part_in[j, span, :].astype(F32)
        square = jnp.sum(residual * residual, axis=1, keepdims=True)
        scaled = (residual * gain_v[:, cols]).astype(BF16)
        return square, jnp.dot(scaled, w_one_v[cols, :], preferred_element_type=F32)

    def score(source, i, square, total):
        for j in range(1, routers):
            more = mixed(source, j)
            square, total = square + more[0], total + more[1]
        norm = lax.rsqrt(square / model + EPSILON)
        hidden = silu(norm * total).astype(BF16)
        sc_out[i] = lax.dot_general(
            two, hidden, (((1,), (1,)), ((), ())), preferred_element_type=F32
        )

    def score_copy(i, e, owner, sem):
        return pltpu.make_async_remote_copy(
            src_ref=sc_out.at[i],
            dst_ref=ret.at[owner],
            send_sem=sc_send.at[i, e],
            recv_sem=sc_recv.at[sem],
            device_id={"users": seat * mine + far_first(seat, i, mine), "heads": e},
            device_id_type=MESH,
        )

    group = mine // 2
    early = {}
    with jax.named_scope("early"):
        for i in range(mine):
            source = far_first(seat, i, mine)
            if i % group == 0:
                drain(po_recv.at[far_first(seat, i // group, 2)], piece * out_cols * 2)
            early[i] = mixed(source, 0)
    for i in range(mine):
        source = far_first(seat, i, mine)
        if i % group == 0:
            with jax.named_scope("partwait"):
                drain(
                    po_recv.at[2 + far_first(seat, i // group, 2)],
                    (routers - 1) * piece * out_cols * 2,
                )
        with jax.named_scope("score"):
            score(source, i, *early[i])
        target = seat * mine + source
        for e in range(heads):
            itself = (target == me) & (h == e)

            @pl.when(jnp.logical_not(itself))
            def _():
                score_copy(i, e, me, me).start()

            @pl.when(itself)
            def _():
                ret[me] = sc_out[i]

    rounds = {"t": 1 + (groups - 1) + groups, "g": groups, "p": 2, "o": 1}
    hops = sum(piece_bytes(t) * rounds[pieces[t][1]] for t in live)
    total = (routers - 1) * hops + (users - 1) * (2 * slot_bytes + mask_bytes)
    drain(sent.at[0], total + size(stat_out) + size(part_out))
    handler = heads - 1 - me // mine
    with jax.named_scope("scorewait"):
        for d in range(users):

            @pl.when(jnp.logical_not((d == me) & (h == handler)))
            def _():
                score_copy(0, 0, d, d).wait_recv()

    position = lax.broadcasted_iota(jnp.int32, (1, width), 1)
    for b in range(blocks):
        tile_in = ret[owners[b]]
        line = tile_in[0:1, 0:width]
        for cap in range(1, CAP):
            line = jnp.where(ranks[b] == cap, tile_in[0:1, cap * width : (cap + 1) * width], line)
        out_ref[b : b + 1, :] = jnp.where(position < fill_ref[b], line, 0.0)

    for i in range(mine):
        for e in range(heads):

            @pl.when(jnp.logical_not((seat * mine + far_first(seat, i, mine) == me) & (h == e)))
            def _():
                score_copy(i, e, me, me).wait_send()


def local(
    sizes,
    items,
    block_owner,
    block_user,
    block_fill,
    prefix_keys,
    prefix_values,
    w_in,
    attn_gain,
    w_o,
    mlp_gain,
    w_one,
    w_two,
):
    groups, users, routers, heads = sizes
    blocks, width, model = items.shape
    projections, depth, half_width = w_in.shape
    slots = users * CAP
    rows = slots * width
    half = rows // heads
    out_cols = w_o.shape[1]
    cached, per_user, _ = prefix_keys.shape
    positions = cached * per_user
    pieces = plan(groups, depth, half_width)
    live = sum(1 for piece in pieces if piece[3])
    trees = sum(1 for piece in pieces if piece[3] and piece[1] == "t")
    dma = pltpu.SemaphoreType.DMA
    yard_bytes = 2 * (
        (routers - 1) * (w_in.size + w_o.size)
        + (users - 1) * (2 * CAP * (width // heads) * model + 2 * 8 * HEAD_DIM)
        + 2 * 2 * rows * 128
        + routers * half * out_cols
    )
    yard_rows = yard_bytes // 256 // 8 * 8
    hbm = pl.BlockSpec(memory_space=pl.ANY)
    vmem = pl.BlockSpec(memory_space=pltpu.VMEM)
    scratch = [
        pltpu.SMEM((blocks,), jnp.int32),
        pltpu.SMEM((blocks,), jnp.int32),
        pltpu.SMEM((blocks,), jnp.int32),
        pltpu.VMEM(attn_gain.shape, BF16),
        pltpu.VMEM(mlp_gain.shape, BF16),
        pltpu.VMEM(w_two.shape, BF16),
        pltpu.VMEM((blocks, width, model), BF16),
        pltpu.VMEM((users, CAP, width // heads, model), BF16),
        pltpu.VMEM((slots, width, model), BF16),
        pltpu.VMEM((users, 8, HEAD_DIM), F32),
        pltpu.VMEM((users, 8, HEAD_DIM), F32),
        pltpu.VMEM(prefix_keys.shape, BF16),
        pltpu.VMEM(prefix_values.shape, BF16),
        pltpu.VMEM((half_width // HEAD_DIM, cached * HEAD_DIM, per_user), BF16),
        pltpu.VMEM((1, model), F32),
        pltpu.VMEM((cached, rows, HEAD_DIM), BF16),
        pltpu.VMEM((rows, half_width), F32),
        pltpu.VMEM((projections, rows, half_width), F32),
        pltpu.VMEM((projections, routers, depth, half_width), BF16),
        pltpu.VMEM((routers, half_width, out_cols), BF16),
        pltpu.VMEM(w_one.shape, BF16),
        pltpu.VMEM((rows, half_width), BF16),
        pltpu.VMEM((rows, half_width), F32),
        pltpu.VMEM((rows, half_width), F32),
        pltpu.VMEM((rows, half_width), BF16),
        pltpu.VMEM((rows // (8 * width), width, 128), F32),
        pltpu.VMEM((rows // (8 * width), width, 128), F32),
        pltpu.VMEM((routers, half, out_cols), BF16),
        pltpu.VMEM((routers, half, out_cols), F32),
        pltpu.VMEM((routers, half, out_cols), BF16),
        pltpu.VMEM((users // heads, 8, CAP * width), F32),
        pltpu.VMEM((users, 8, CAP * width), F32),
        dma((11,)),
        dma((1,)),
        dma((users - 1,)),
        dma((3,)),
        dma((routers - 1, live)),
        dma((groups - 1, routers - 1, 5 + trees)),
        dma((routers - 1, 5)),
        dma((rows // (8 * width),)),
        dma((4,)),
        dma((users // heads, heads)),
        dma((users,)),
        pltpu.VMEM((yard_rows, 128), BF16),
    ]
    return pl.pallas_call(
        functools.partial(scorer, sizes),
        out_shape=pltpu.VMEM((blocks, width), F32),
        in_specs=[hbm] * 12,
        out_specs=vmem,
        scratch_shapes=scratch,
        compiler_params=pltpu.CompilerParams(
            collective_id=0, has_side_effects=True, vmem_limit_bytes=62 * 1024 * 1024
        ),
    )(
        items,
        block_owner.reshape(-1),
        block_user,
        block_fill,
        prefix_keys,
        prefix_values,
        w_in,
        attn_gain,
        w_o,
        mlp_gain,
        w_one,
        w_two,
    )


def solution(mesh):
    placed = (
        P(("groups", "users", "routers"), None, None),
        P(("groups", "users", "routers"), None),
        P(("groups", "users", "routers")),
        P(("groups", "users", "routers")),
        P(("groups", "users"), None, "heads"),
        P(("groups", "users"), None, "heads"),
        P(None, "routers", "heads"),
        P("heads"),
        P("heads", "routers"),
        P(),
        P(),
        P(),
    )
    sizes = tuple(mesh.shape[name] for name in ("groups", "users", "routers", "heads"))
    return jax.shard_map(
        functools.partial(local, sizes),
        mesh=mesh,
        in_specs=placed,
        out_specs=P(("groups", "users", "routers"), None),
        check_vma=False,
    )
```

```python
import functools
import math

import jax
import jax.numpy as jnp
from jax import lax
from jax.experimental import pallas as pl
from jax.experimental.pallas import tpu as pltpu
from jax.sharding import PartitionSpec as P

HEAD_DIM = 128
CAP = 2
EPSILON = 1e-05
UNIT = 512
PIECES = (
    (1, "t", 112),
    (0, "g", 80),
    (2, "t", 80),
    (0, "g", 80),
    (0, "g", 96),
    (3, "t", 64),
    (1, "g", 32),
    (3, "t", 32),
    (2, "g", 96),
    (3, "g", 64),
    (4, "g", 96),
    (4, "p", 48),
    (4, "p", 32),
    (4, "o", 160),
    (3, "o", 0),
    (2, "o", 0),
    (1, "o", 0),
    (0, "o", 0),
)
STEPS = (
    "T", "f0", "f1", "f2", "r1", "r2", "z0", "f3", "f4", "r3", "z2", "f5", "f6", "rA", "rB", "f7",
    "p0", "p1", "p2", "p3", "f8", "L0", "q", "a0", "f9", "z5", "a1", "L1", "k", "z7", "f10", "f11",
    "f12", "L2", "v", "L3", "g0", "g1", "o0", "L4", "o1",
)
F32 = jnp.float32
BF16 = jnp.bfloat16
MESH = pl.DeviceIdType.MESH


def silu(v):
    return 0.5 * v * (1.0 + jnp.tanh(0.5 * v))


def plan(groups, depth, half_width):
    copies = {"t": groups * 2, "g": groups, "p": 2, "o": 1}
    lengths = [depth] * 4 + [half_width]
    filled = [0] * 5
    pieces = []
    for p, kind, share in PIECES:
        count = 0 if kind == "o" else share * lengths[p] // UNIT // 16 * 16
        pieces.append([p, kind, filled[p], count])
        filled[p] += copies[kind] * count
    for n, piece in enumerate(pieces):
        p = piece[0]
        if piece[1] == "o":
            left = lengths[p] - filled[p]
            if any(q[:2] == piece[:2] for q in pieces[n + 1 :]):
                left = min(left, PIECES[n][2] * lengths[p] // UNIT // 16 * 16)
            piece[2:] = filled[p], left
            filled[p] += left
    return pieces


def scorer(
    sizes,
    items_ref,
    owner_hbm,
    user_hbm,
    fill_hbm,
    keys_ref,
    values_ref,
    w_in_ref,
    attn_gain_hbm,
    w_o_ref,
    mlp_gain_hbm,
    w_one_ref,
    w_two_hbm,
    out_ref,
    owner_ref,
    user_ref,
    fill_ref,
    attn_gain_ref,
    mlp_gain_ref,
    w_two_ref,
    items_v,
    out_slots,
    x_all,
    mask_out,
    mask_all,
    keys_v,
    values_v,
    turned,
    gain_v,
    pick_v,
    gate_v,
    pre_v,
    w_all,
    wo_all,
    w_one_v,
    q_v,
    own_v,
    att_v,
    gated_v,
    stat_out,
    stat_in,
    part_out,
    part_own,
    part_in,
    sc_out,
    ret,
    local_sem,
    sent,
    z_recv,
    group_recv,
    x_recv,
    y_recv,
    w_recv,
    st_recv,
    po_recv,
    sc_send,
    sc_recv,
    yard,
):
    groups, users, routers, heads = sizes
    g = lax.axis_index("groups")
    me = lax.axis_index("users")
    r = lax.axis_index("routers")
    h = lax.axis_index("heads")
    mate = 1 - h
    blocks, width, model = items_v.shape
    slots = x_all.shape[0]
    half_width = q_v.shape[1]
    heads_here = half_width // HEAD_DIM
    hd_all = half_width * heads
    rows = slots * width
    depth = w_all.shape[2]
    out_cols = wo_all.shape[2]
    wh = width // heads
    scale = HEAD_DIM ** (-0.5)
    positions = keys_v.shape[0] * keys_v.shape[1]
    per_user = keys_v.shape[1]

    barrier = pltpu.get_barrier_semaphore()
    count = 0
    for j in range(1, routers):
        pl.semaphore_signal(
            barrier, inc=1, device_id={"routers": lax.rem(r + j, routers)}, device_id_type=MESH
        )
        count += 1
    for i in range(1, groups):
        pl.semaphore_signal(
            barrier, inc=1, device_id={"groups": lax.rem(g + i, groups)}, device_id_type=MESH
        )
        count += 1
    pl.semaphore_signal(barrier, inc=1, device_id={"heads": mate}, device_id_type=MESH)
    count += 1
    for k in range(1, users):
        for e in range(heads):
            pl.semaphore_signal(
                barrier,
                inc=1,
                device_id={"users": lax.rem(me + k, users), "heads": e},
                device_id_type=MESH,
            )
            count += 1
    first = [
        pltpu.make_async_copy(src, dst, local_sem.at[n])
        for n, (src, dst) in enumerate(
            (
                (owner_hbm, owner_ref),
                (user_hbm, user_ref),
                (fill_hbm, fill_ref),
                (items_ref, items_v),
            )
        )
    ]
    gains = [
        pltpu.make_async_copy(src, dst, local_sem.at[4 + n])
        for n, (src, dst) in enumerate(
            (
                (attn_gain_hbm, attn_gain_ref),
                (mlp_gain_hbm, mlp_gain_ref),
                (w_two_hbm, w_two_ref),
            )
        )
    ]
    order = [p for p, _, _ in PIECES]
    ahead = list(dict.fromkeys(order))[:2]
    opening = min(t for t, p in enumerate(order) if p not in ahead)
    lead = [
        pltpu.make_async_copy(w_in_ref.at[p], w_all.at[p, r], local_sem.at[8 + n])
        for n, p in enumerate(ahead)
    ]
    later = [p for p in range(4) if p not in ahead]
    bulk = [
        pltpu.make_async_copy(src, dst, local_sem.at[7])
        for src, dst in [(w_in_ref.at[p], w_all.at[p, r]) for p in later]
        + [(w_o_ref, wo_all.at[r])]
    ]
    rest = [
        pltpu.make_async_copy(src, dst, local_sem.at[10])
        for src, dst in ((keys_ref, keys_v), (values_ref, values_v), (w_one_ref, w_one_v))
    ]

    def size(*refs):
        return sum(math.prod(ref.shape) * jnp.dtype(ref.dtype).itemsize for ref in refs)

    def drain(sem, amount):
        part = yard.at[pl.ds(0, amount // (yard.shape[1] * 2)), :]
        pltpu.make_async_copy(part, part, sem).wait()

    for c in lead + first + bulk:
        c.start()
    pl.semaphore_wait(barrier, count)

    pieces = plan(groups, depth, half_width)
    live = [t for t in range(len(pieces)) if pieces[t][3]]
    slot_x = {t: n for n, t in enumerate(live)}
    slot_y = {t: n + 5 for n, t in enumerate(t for t in live if pieces[t][1] == "t")}
    slot_y.update({t: pieces[t][0] for t in live if pieces[t][1] == "g"})
    parity = lax.rem(me, 2)
    pair = me + 1 - 2 * parity

    def weight_slot(owner_router, owner_group, owner_parity, t):
        p, kind, start, length = pieces[t]
        index = {
            "t": owner_group * 2 + owner_parity,
            "g": owner_group,
            "p": owner_parity,
            "o": 0,
        }[kind]
        start = start + index * length
        if kind != "o":
            start = pl.multiple_of(start, 16)
        span = pl.ds(start, length)
        if p < 4:
            return w_all.at[p, owner_router, span, :]
        return wo_all.at[owner_router, span, :]

    def piece_bytes(t):
        return size(weight_slot(0, 0, 0, t))

    def x_copy(j, t, source_router):
        spot = weight_slot(source_router, g, parity, t)
        return pltpu.make_async_remote_copy(
            src_ref=spot,
            dst_ref=spot,
            send_sem=sent.at[0],
            recv_sem=x_recv.at[j - 1, slot_x[t]],
            device_id={"routers": lax.rem(r + j, routers)},
            device_id_type=MESH,
        )

    def y_copy(i, j, t, owner_group):
        spot = weight_slot(lax.rem(r - j + routers, routers), owner_group, parity, t)
        return pltpu.make_async_remote_copy(
            src_ref=spot,
            dst_ref=spot,
            send_sem=sent.at[0],
            recv_sem=y_recv.at[i - 1, j - 1, slot_y[t]],
            device_id={"groups": lax.rem(g + i, groups)},
            device_id_type=MESH,
        )

    def pair_copy(i, j, t):
        spot = weight_slot(
            lax.rem(r - j + routers, routers), lax.rem(g - i + groups, groups), parity, t
        )
        return pltpu.make_async_remote_copy(
            src_ref=spot,
            dst_ref=spot,
            send_sem=sent.at[0],
            recv_sem=w_recv.at[j - 1, pieces[t][0]],
            device_id={"users": pair},
            device_id_type=MESH,
        )

    def send_x(t):
        if t in live:
            for j in range(1, routers):
                x_copy(j, t, r).start()

    def send_first():
        lead[0].wait()
        for t in range(opening):
            if order[t] != ahead[0] and ahead[1] not in order[:t]:
                lead[1].wait()
            send_x(t)

    send_first()
    for c in first[:3]:
        c.wait()
    owners = [owner_ref[b] for b in range(blocks)]
    ranks = []
    for b in range(blocks):
        rank = jnp.int32(0)
        for a in range(b):
            rank = rank + jnp.where(owners[a] == owners[b], 1, 0)
        ranks.append(rank)

    def slot_source(dest, cap):
        index, user = jnp.int32(0), jnp.int32(-1)
        for b in range(blocks):
            hit = (owners[b] == dest) & (ranks[b] == cap)
            index = jnp.where(hit, b, index)
            user = jnp.where(hit, user_ref[b], user)
        return index, user

    mask_bytes = size(mask_out) // users
    slot_bytes = size(out_slots) // users
    cached = keys_v.shape[0]
    row_user = lax.broadcasted_iota(jnp.int32, (8, HEAD_DIM), 0)
    mask_copies, item_copies = {}, {}

    def across(k):
        other = me
        bit = 1
        while bit < users:
            if k & bit:
                other = other + bit - 2 * bit * lax.rem(me // bit, 2)
            bit *= 2
        return other

    def z_copy(k, source):
        return pltpu.make_async_remote_copy(
            src_ref=out_slots.at[k],
            dst_ref=x_all.at[pl.ds(source * CAP, CAP), pl.ds(pl.multiple_of(h * wh, wh), wh), :],
            send_sem=sent.at[0],
            recv_sem=z_recv.at[k - 1],
            device_id={"users": across(k)},
            device_id_type=MESH,
        )

    def m_copy(k, source):
        return pltpu.make_async_remote_copy(
            src_ref=mask_out.at[k],
            dst_ref=mask_all.at[source],
            send_sem=sent.at[0],
            recv_sem=group_recv.at[0],
            device_id={"users": across(k)},
            device_id_type=MESH,
        )

    def relay_copy(k, part):
        spot = x_all.at[
            pl.ds(across(k) * CAP, CAP), pl.ds(pl.multiple_of(part * wh, wh), wh), :
        ]
        return pltpu.make_async_remote_copy(
            src_ref=spot,
            dst_ref=spot,
            send_sem=sent.at[0],
            recv_sem=group_recv.at[2 if k == 1 else 1],
            device_id={"heads": mate},
            device_id_type=MESH,
        )

    for k in list(range(1, users)) + [0]:
        lines = jnp.zeros((8, HEAD_DIM), F32)
        for cap in range(CAP):
            user = slot_source(across(k), cap)[1]
            lines = lines + jnp.where(row_user == user + cap * cached, jnp.where(user < 0, 0.0, 1.0), 0.0)
        if k:
            mask_out[k] = lines
            m_copy(k, me).start()
        else:
            mask_all[me] = lines
    first[3].wait()
    for k in list(range(1, users)) + [0]:
        for cap in range(CAP):
            index = slot_source(across(k), cap)[0]
            if k:
                out_slots[k, cap] = items_v[index, pl.ds(pl.multiple_of(h * wh, wh), wh), :]
            else:
                x_all[me * CAP + cap] = items_v[index]
        if k:
            z_copy(k, me).start()
    drain(local_sem.at[7], size(w_o_ref) + len(later) * (size(w_in_ref) // 4))
    for t in range(opening, len(pieces)):
        send_x(t)
    for c in rest + gains:
        c.start()

    def forward(t):
        if t not in live:
            return
        kind = pieces[t][1]
        for j in range(1, routers):
            x_copy(j, t, lax.rem(r - j + routers, routers)).wait_recv()
            if kind in "tg":
                for i in range(1, groups):
                    y_copy(i, j, t, g).start()
            if kind in "tp":
                pair_copy(0, j, t).start()

    def second(t):
        if t not in live:
            return
        for j in range(1, routers):
            for i in range(1, groups):
                y_copy(i, j, t, lax.rem(g - i + groups, groups)).wait_recv()
                pair_copy(i, j, t).start()

    def landed(p):
        mine_of = [t for t in live if pieces[t][0] == p]
        straight = sum(piece_bytes(t) for t in mine_of if pieces[t][1] == "g")
        paired = sum(
            piece_bytes(t) * (groups if pieces[t][1] == "t" else 1)
            for t in mine_of
            if pieces[t][1] in "tp"
        )
        for j in range(1, routers):
            for t in mine_of:
                if pieces[t][1] == "o":
                    x_copy(j, t, lax.rem(r - j + routers, routers)).wait_recv()
            for i in range(1, groups):
                if straight:
                    drain(y_recv.at[i - 1, j - 1, p], straight)
            if paired:
                drain(w_recv.at[j - 1, p], paired)

    tile_slots = 4
    tile = tile_slots * width

    wide = 2 * tile

    def wide_span(i):
        return pl.ds(pl.multiple_of(i * wide, wide), wide)

    def product(p, i, a):
        cols = pl.ds(pl.multiple_of(a * depth, depth), depth)
        x = x_all[pl.ds(i * 2 * tile_slots, 2 * tile_slots), :, cols]
        return jnp.dot(x.reshape(wide, depth), w_all[p, a], preferred_element_type=F32)

    def prepare(i, p):
        pre_v[p, wide_span(i), :] = product(p, i, r)

    def projected(p, i):
        total = pre_v[p, wide_span(i), :]
        for j in range(1, routers):
            total = total + product(p, i, lax.rem(r - j + routers, routers))
        return silu(total)

    def query(i):
        q_v[wide_span(i), :] = projected(0, i).astype(BF16)

    def turn():
        gain_v[...] = mlp_gain_ref[...].astype(F32).reshape(1, -1)
        for e in range(heads_here):
            for u in range(cached):
                turned[e, u * HEAD_DIM : (u + 1) * HEAD_DIM, :] = keys_v[
                    u, :, e * HEAD_DIM : (e + 1) * HEAD_DIM
                ].T

    def picking(i):
        for s in range(2 * tile_slots):
            for u in range(cached):
                spot = s % CAP * cached + u
                line = mask_all[i * (2 * tile_slots // CAP) + s // CAP, spot : spot + 1, :]
                rows_s = pl.ds(pl.multiple_of(i * wide + s * width, width), width)
                pick_v[u, rows_s, :] = jnp.broadcast_to(line, (width, HEAD_DIM)).astype(BF16)

    def attend(i, part):
        span = wide_span(i)
        picks = [pick_v[u, span, :] for u in range(cached)]
        share = heads_here // 2
        for e in range(part * share, (part + 1) * share):
            cols = slice(e * HEAD_DIM, (e + 1) * HEAD_DIM)
            q = q_v[span, cols]
            raw = jnp.dot(
                jnp.concatenate([q * pick for pick in picks], axis=1),
                turned[e],
                preferred_element_type=F32,
            )
            weights = silu(raw * scale).astype(BF16)
            times = per_user // HEAD_DIM
            weights = jnp.concatenate(
                [weights * jnp.concatenate([pick] * times, axis=1) for pick in picks], axis=1
            )
            att_v[span, cols] = (
                jnp.dot(
                    weights,
                    values_v[:, :, cols].reshape(positions, HEAD_DIM),
                    preferred_element_type=F32,
                )
                .astype(BF16)
                .astype(F32)
            )

    def self_key(i):
        span = wide_span(i)
        keys = projected(1, i)
        for e in range(heads_here):
            cols = slice(e * HEAD_DIM, (e + 1) * HEAD_DIM)
            own = jnp.sum(q_v[span, cols].astype(F32) * keys[:, cols], axis=1, keepdims=True)
            own_v[span, cols] = jnp.broadcast_to(silu(own * scale), (wide, HEAD_DIM))

    lane = lax.broadcasted_iota(jnp.int32, (width, 128), 1)

    def self_value(i):
        span = wide_span(i)
        att = att_v[span, :] + own_v[span, :] * projected(2, i)
        att_v[span, :] = att
        total = jnp.sum(att, axis=1, keepdims=True)
        square = jnp.sum(att * att, axis=1, keepdims=True)
        packed = jnp.zeros((width, 128), F32)
        for b in range(wide // width):
            part = slice(b * width, (b + 1) * width)
            packed = jnp.where(lane == 2 * b, total[part], packed)
            packed = jnp.where(lane == 2 * b + 1, square[part], packed)
        stat_out[i] = packed

    def gate(i):
        gate_v[wide_span(i), :] = attn_gain_ref[...].astype(F32).reshape(1, -1) * projected(3, i)

    def gating(i):
        stat_copy(i).wait_recv()
        both = stat_out[i] + stat_in[i]
        for b in range(wide // width):
            span = pl.ds(pl.multiple_of(i * wide + b * width, width), width)
            mean = both[:, 2 * b : 2 * b + 1] / hd_all
            var = both[:, 2 * b + 1 : 2 * b + 2] / hd_all - mean * mean
            gated_v[span, :] = (
                (att_v[span, :] - mean) * lax.rsqrt(var + EPSILON) * gate_v[span, :]
            ).astype(BF16)

    def stat_copy(i):
        return pltpu.make_async_remote_copy(
            src_ref=stat_out.at[i],
            dst_ref=stat_in.at[i],
            send_sem=sent.at[0],
            recv_sem=st_recv.at[i],
            device_id={"heads": mate},
            device_id_type=MESH,
        )

    def value(i):
        self_value(i)
        stat_copy(i).start()

    def whole(fun):
        for i in range(rows // wide):
            fun(i)

    half = rows // heads

    mine = users // heads
    seat, seat_mate = heads - 1 - h, heads - 1 - mate
    piece = half // 2
    source_rows = CAP * width

    def far_first(e, i, amount):
        return jnp.where(me < e * mine + mine // 2, amount - 1 - i, i)

    def part_copy(j, c):
        spot = pl.ds(pl.multiple_of(c * piece, piece), piece)
        return pltpu.make_async_remote_copy(
            src_ref=part_out.at[j, spot, :],
            dst_ref=part_in.at[j, spot, :],
            send_sem=sent.at[0],
            recv_sem=po_recv.at[c if j == 0 else 2 + c],
            device_id={"heads": mate},
            device_id_type=MESH,
        )

    def shares(j):
        pieces_of = (half,) if j == 0 else (piece, piece)
        for i, count in enumerate(pieces_of):
            c = 0 if j == 0 else far_first(seat_mate, i, 2)
            start = pl.multiple_of(c * piece, piece)
            part_out[j, pl.ds(start, count), :] = jnp.dot(
                gated_v[pl.ds(pl.multiple_of(seat_mate * half + start, piece), count), :],
                wo_all[lax.rem(r - j + routers, routers)],
                preferred_element_type=F32,
            ).astype(BF16)
            if j:
                part_copy(j, c).start()
        if j == 0:
            for i in range(2):
                part_copy(j, far_first(seat_mate, i, 2)).start()

    def outer(js):
        for j in js:
            shares(j)
        for j in js:
            part_own[j] = jnp.dot(
                gated_v[pl.ds(pl.multiple_of(seat * half, half), half), :],
                wo_all[lax.rem(r - j + routers, routers)],
                preferred_element_type=F32,
            )

    def step(name):
        if name == "T":
            drain(local_sem.at[10], size(keys_ref, values_ref, w_one_ref))
            for c in gains:
                c.wait()
            turn()
        elif name[0] == "f":
            forward(int(name[1:]))
        elif name[0] == "z":
            second(int(name[1:]))
        elif name[0] == "L":
            landed(int(name[1:]))
        elif name[0] == "r" and name[1] in "AB":
            if name[1] == "A":
                drain(group_recv.at[2], slot_bytes)
                drain(group_recv.at[0], (users - 1) * mask_bytes)
                whole(picking)
            else:
                drain(group_recv.at[1], (users - 2) * slot_bytes)
        elif name[0] == "r":
            for k in range(int(name[1:]), users if name == "r3" else int(name[1:]) + 1):
                z_copy(k, across(k)).wait_recv()
                relay_copy(k, h).start()
        elif name[0] == "p":
            whole(functools.partial(prepare, p=int(name[1])))
        elif name[0] == "q":
            whole(query)
        elif name[0] == "a":
            whole(functools.partial(attend, part=int(name[1])))
        elif name[0] == "k":
            whole(self_key)
        elif name[0] == "v":
            whole(value)
        elif name == "g0":
            whole(gate)
        elif name == "g1":
            whole(gating)
        elif name == "o0":
            outer([0])
        else:
            outer(range(1, routers))

    for name in STEPS:
        with jax.named_scope(name):
            step(name)

    two = jnp.broadcast_to(
        w_two_ref[...].astype(F32).reshape(1, -1), (8, w_two_ref.shape[0])
    ).astype(BF16)

    def mixed(source, j):
        a = lax.rem(r - j + routers, routers)
        span = pl.ds(pl.multiple_of(source * source_rows, source_rows), source_rows)
        cols = pl.ds(pl.multiple_of(a * out_cols, out_cols), out_cols)
        x = x_all[pl.ds((seat * mine + source) * CAP, CAP), :, cols]
        x = x.reshape(source_rows, out_cols).astype(F32)
        residual = x + part_own[j, span, :] + part_in[j, span, :].astype(F32)
        square = jnp.sum(residual * residual, axis=1, keepdims=True)
        scaled = (residual * gain_v[:, cols]).astype(BF16)
        return square, jnp.dot(scaled, w_one_v[cols, :], preferred_element_type=F32)

    def score(source, i, square, total):
        for j in range(1, routers):
            more = mixed(source, j)
            square, total = square + more[0], total + more[1]
        norm = lax.rsqrt(square / model + EPSILON)
        hidden = silu(norm * total).astype(BF16)
        sc_out[i] = lax.dot_general(
            two, hidden, (((1,), (1,)), ((), ())), preferred_element_type=F32
        )

    def score_copy(i, e, owner, sem):
        return pltpu.make_async_remote_copy(
            src_ref=sc_out.at[i],
            dst_ref=ret.at[owner],
            send_sem=sc_send.at[i, e],
            recv_sem=sc_recv.at[sem],
            device_id={"users": seat * mine + far_first(seat, i, mine), "heads": e},
            device_id_type=MESH,
        )

    group = mine // 2
    early = {}
    with jax.named_scope("early"):
        for i in range(mine):
            source = far_first(seat, i, mine)
            if i % group == 0:
                drain(po_recv.at[far_first(seat, i // group, 2)], piece * out_cols * 2)
            early[i] = mixed(source, 0)
    for i in range(mine):
        source = far_first(seat, i, mine)
        if i % group == 0:
            with jax.named_scope("partwait"):
                drain(
                    po_recv.at[2 + far_first(seat, i // group, 2)],
                    (routers - 1) * piece * out_cols * 2,
                )
        with jax.named_scope("score"):
            score(source, i, *early[i])
        target = seat * mine + source
        for e in range(heads):
            itself = (target == me) & (h == e)

            @pl.when(jnp.logical_not(itself))
            def _():
                score_copy(i, e, me, me).start()

            @pl.when(itself)
            def _():
                ret[me] = sc_out[i]

    rounds = {"t": 1 + (groups - 1) + groups, "g": groups, "p": 2, "o": 1}
    hops = sum(piece_bytes(t) * rounds[pieces[t][1]] for t in live)
    total = (routers - 1) * hops + (users - 1) * (2 * slot_bytes + mask_bytes)
    drain(sent.at[0], total + size(stat_out) + size(part_out))
    handler = heads - 1 - me // mine
    with jax.named_scope("scorewait"):
        for d in range(users):

            @pl.when(jnp.logical_not((d == me) & (h == handler)))
            def _():
                score_copy(0, 0, d, d).wait_recv()

    position = lax.broadcasted_iota(jnp.int32, (1, width), 1)
    for b in range(blocks):
        tile_in = ret[owners[b]]
        line = tile_in[0:1, 0:width]
        for cap in range(1, CAP):
            line = jnp.where(ranks[b] == cap, tile_in[0:1, cap * width : (cap + 1) * width], line)
        out_ref[b : b + 1, :] = jnp.where(position < fill_ref[b], line, 0.0)

    for i in range(mine):
        for e in range(heads):

            @pl.when(jnp.logical_not((seat * mine + far_first(seat, i, mine) == me) & (h == e)))
            def _():
                score_copy(i, e, me, me).wait_send()


def local(
    sizes,
    items,
    block_owner,
    block_user,
    block_fill,
    prefix_keys,
    prefix_values,
    w_in,
    attn_gain,
    w_o,
    mlp_gain,
    w_one,
    w_two,
):
    groups, users, routers, heads = sizes
    blocks, width, model = items.shape
    projections, depth, half_width = w_in.shape
    slots = users * CAP
    rows = slots * width
    half = rows // heads
    out_cols = w_o.shape[1]
    cached, per_user, _ = prefix_keys.shape
    positions = cached * per_user
    pieces = plan(groups, depth, half_width)
    live = sum(1 for piece in pieces if piece[3])
    trees = sum(1 for piece in pieces if piece[3] and piece[1] == "t")
    dma = pltpu.SemaphoreType.DMA
    yard_bytes = 2 * (
        (routers - 1) * (w_in.size + w_o.size)
        + (users - 1) * (2 * CAP * (width // heads) * model + 2 * 8 * HEAD_DIM)
        + 2 * 2 * rows * 128
        + routers * half * out_cols
    )
    yard_rows = yard_bytes // 256 // 8 * 8
    hbm = pl.BlockSpec(memory_space=pl.ANY)
    vmem = pl.BlockSpec(memory_space=pltpu.VMEM)
    scratch = [
        pltpu.SMEM((blocks,), jnp.int32),
        pltpu.SMEM((blocks,), jnp.int32),
        pltpu.SMEM((blocks,), jnp.int32),
        pltpu.VMEM(attn_gain.shape, BF16),
        pltpu.VMEM(mlp_gain.shape, BF16),
        pltpu.VMEM(w_two.shape, BF16),
        pltpu.VMEM((blocks, width, model), BF16),
        pltpu.VMEM((users, CAP, width // heads, model), BF16),
        pltpu.VMEM((slots, width, model), BF16),
        pltpu.VMEM((users, 8, HEAD_DIM), F32),
        pltpu.VMEM((users, 8, HEAD_DIM), F32),
        pltpu.VMEM(prefix_keys.shape, BF16),
        pltpu.VMEM(prefix_values.shape, BF16),
        pltpu.VMEM((half_width // HEAD_DIM, cached * HEAD_DIM, per_user), BF16),
        pltpu.VMEM((1, model), F32),
        pltpu.VMEM((cached, rows, HEAD_DIM), BF16),
        pltpu.VMEM((rows, half_width), F32),
        pltpu.VMEM((projections, rows, half_width), F32),
        pltpu.VMEM((projections, routers, depth, half_width), BF16),
        pltpu.VMEM((routers, half_width, out_cols), BF16),
        pltpu.VMEM(w_one.shape, BF16),
        pltpu.VMEM((rows, half_width), BF16),
        pltpu.VMEM((rows, half_width), F32),
        pltpu.VMEM((rows, half_width), F32),
        pltpu.VMEM((rows, half_width), BF16),
        pltpu.VMEM((rows // (8 * width), width, 128), F32),
        pltpu.VMEM((rows // (8 * width), width, 128), F32),
        pltpu.VMEM((routers, half, out_cols), BF16),
        pltpu.VMEM((routers, half, out_cols), F32),
        pltpu.VMEM((routers, half, out_cols), BF16),
        pltpu.VMEM((users // heads, 8, CAP * width), F32),
        pltpu.VMEM((users, 8, CAP * width), F32),
        dma((11,)),
        dma((1,)),
        dma((users - 1,)),
        dma((3,)),
        dma((routers - 1, live)),
        dma((groups - 1, routers - 1, 5 + trees)),
        dma((routers - 1, 5)),
        dma((rows // (8 * width),)),
        dma((4,)),
        dma((users // heads, heads)),
        dma((users,)),
        pltpu.VMEM((yard_rows, 128), BF16),
    ]
    return pl.pallas_call(
        functools.partial(scorer, sizes),
        out_shape=pltpu.VMEM((blocks, width), F32),
        in_specs=[hbm] * 12,
        out_specs=vmem,
        scratch_shapes=scratch,
        compiler_params=pltpu.CompilerParams(
            collective_id=0, has_side_effects=True, vmem_limit_bytes=62 * 1024 * 1024
        ),
    )(
        items,
        block_owner.reshape(-1),
        block_user,
        block_fill,
        prefix_keys,
        prefix_values,
        w_in,
        attn_gain,
        w_o,
        mlp_gain,
        w_one,
        w_two,
    )


def solution(mesh):
    placed = (
        P(("groups", "users", "routers"), None, None),
        P(("groups", "users", "routers"), None),
        P(("groups", "users", "routers")),
        P(("groups", "users", "routers")),
        P(("groups", "users"), None, "heads"),
        P(("groups", "users"), None, "heads"),
        P(None, "routers", "heads"),
        P("heads"),
        P("heads", "routers"),
        P(),
        P(),
        P(),
    )
    sizes = tuple(mesh.shape[name] for name in ("groups", "users", "routers", "heads"))
    return jax.shard_map(
        functools.partial(local, sizes),
        mesh=mesh,
        in_specs=placed,
        out_specs=P(("groups", "users", "routers"), None),
        check_vma=False,
    )
```

```python
import functools
import math

import jax
import jax.numpy as jnp
from jax import lax
from jax.experimental import pallas as pl
from jax.experimental.pallas import tpu as pltpu
from jax.sharding import PartitionSpec as P

HEAD_DIM = 128
CAP = 2
EPSILON = 1e-05
UNIT = 512
PIECES = (
    (1, "t", 112),
    (0, "g", 80),
    (2, "t", 80),
    (0, "g", 80),
    (0, "g", 96),
    (3, "t", 64),
    (1, "g", 32),
    (3, "t", 32),
    (2, "g", 96),
    (3, "g", 64),
    (4, "g", 96),
    (4, "p", 48),
    (4, "p", 32),
    (4, "o", 160),
    (3, "o", 0),
    (2, "o", 0),
    (1, "o", 0),
    (0, "o", 0),
)
STEPS = (
    "T", "f0", "f1", "f2", "r1", "r2", "z0", "f3", "f4", "r3", "z2", "f5", "f6", "rA", "rB", "f7",
    "p0", "p1", "p2", "p3", "f8", "L0", "q", "a0", "f9", "z5", "a1", "L1", "k", "z7", "f10", "f11",
    "f12", "L2", "v", "L3", "g0", "g1", "o0", "L4", "o1",
)
F32 = jnp.float32
BF16 = jnp.bfloat16
MESH = pl.DeviceIdType.MESH


def silu(v):
    return 0.5 * v * (1.0 + jnp.tanh(0.5 * v))


def plan(groups, depth, half_width):
    copies = {"t": groups * 2, "g": groups, "p": 2, "o": 1}
    lengths = [depth] * 4 + [half_width]
    filled = [0] * 5
    pieces = []
    for p, kind, share in PIECES:
        count = 0 if kind == "o" else share * lengths[p] // UNIT // 16 * 16
        pieces.append([p, kind, filled[p], count])
        filled[p] += copies[kind] * count
    for n, piece in enumerate(pieces):
        p = piece[0]
        if piece[1] == "o":
            left = lengths[p] - filled[p]
            if any(q[:2] == piece[:2] for q in pieces[n + 1 :]):
                left = min(left, PIECES[n][2] * lengths[p] // UNIT // 16 * 16)
            piece[2:] = filled[p], left
            filled[p] += left
    return pieces


def scorer(
    sizes,
    items_ref,
    owner_hbm,
    user_hbm,
    fill_hbm,
    keys_ref,
    values_ref,
    w_in_ref,
    attn_gain_hbm,
    w_o_ref,
    mlp_gain_hbm,
    w_one_ref,
    w_two_hbm,
    out_ref,
    owner_ref,
    user_ref,
    fill_ref,
    attn_gain_ref,
    mlp_gain_ref,
    w_two_ref,
    items_v,
    out_slots,
    x_all,
    mask_out,
    mask_all,
    keys_v,
    values_v,
    turned,
    gain_v,
    pick_v,
    gate_v,
    pre_v,
    w_all,
    wo_all,
    w_one_v,
    q_v,
    own_v,
    att_v,
    gated_v,
    stat_out,
    stat_in,
    part_out,
    part_own,
    part_in,
    sc_out,
    ret,
    local_sem,
    sent,
    z_recv,
    group_recv,
    x_recv,
    y_recv,
    w_recv,
    st_recv,
    po_recv,
    sc_send,
    sc_recv,
    yard,
):
    groups, users, routers, heads = sizes
    g = lax.axis_index("groups")
    me = lax.axis_index("users")
    r = lax.axis_index("routers")
    h = lax.axis_index("heads")
    mate = 1 - h
    blocks, width, model = items_v.shape
    slots = x_all.shape[0]
    half_width = q_v.shape[1]
    heads_here = half_width // HEAD_DIM
    hd_all = half_width * heads
    rows = slots * width
    depth = w_all.shape[2]
    out_cols = wo_all.shape[2]
    wh = width // heads
    scale = HEAD_DIM ** (-0.5)
    positions = keys_v.shape[0] * keys_v.shape[1]
    per_user = keys_v.shape[1]

    barrier = pltpu.get_barrier_semaphore()
    count = 0
    for j in range(1, routers):
        pl.semaphore_signal(
            barrier, inc=1, device_id={"routers": lax.rem(r + j, routers)}, device_id_type=MESH
        )
        count += 1
    for i in range(1, groups):
        pl.semaphore_signal(
            barrier, inc=1, device_id={"groups": lax.rem(g + i, groups)}, device_id_type=MESH
        )
        count += 1
    pl.semaphore_signal(barrier, inc=1, device_id={"heads": mate}, device_id_type=MESH)
    count += 1
    for k in range(1, users):
        for e in range(heads):
            pl.semaphore_signal(
                barrier,
                inc=1,
                device_id={"users": lax.rem(me + k, users), "heads": e},
                device_id_type=MESH,
            )
            count += 1
    first = [
        pltpu.make_async_copy(src, dst, local_sem.at[n])
        for n, (src, dst) in enumerate(
            (
                (owner_hbm, owner_ref),
                (user_hbm, user_ref),
                (fill_hbm, fill_ref),
                (items_ref, items_v),
            )
        )
    ]
    gains = [
        pltpu.make_async_copy(src, dst, local_sem.at[4 + n])
        for n, (src, dst) in enumerate(
            (
                (attn_gain_hbm, attn_gain_ref),
                (mlp_gain_hbm, mlp_gain_ref),
                (w_two_hbm, w_two_ref),
            )
        )
    ]
    order = [p for p, _, _ in PIECES]
    ahead = list(dict.fromkeys(order))[:2]
    opening = min(t for t, p in enumerate(order) if p not in ahead)
    lead = [
        pltpu.make_async_copy(w_in_ref.at[p], w_all.at[p, r], local_sem.at[8 + n])
        for n, p in enumerate(ahead)
    ]
    later = [p for p in range(4) if p not in ahead]
    bulk = [
        pltpu.make_async_copy(src, dst, local_sem.at[7])
        for src, dst in [(w_in_ref.at[p], w_all.at[p, r]) for p in later]
        + [(w_o_ref, wo_all.at[r])]
    ]
    rest = [
        pltpu.make_async_copy(src, dst, local_sem.at[10])
        for src, dst in ((keys_ref, keys_v), (values_ref, values_v), (w_one_ref, w_one_v))
    ]

    def size(*refs):
        return sum(math.prod(ref.shape) * jnp.dtype(ref.dtype).itemsize for ref in refs)

    def drain(sem, amount):
        part = yard.at[pl.ds(0, amount // (yard.shape[1] * 2)), :]
        pltpu.make_async_copy(part, part, sem).wait()

    for c in lead + first + bulk:
        c.start()
    pl.semaphore_wait(barrier, count)

    pieces = plan(groups, depth, half_width)
    live = [t for t in range(len(pieces)) if pieces[t][3]]
    slot_x = {t: n for n, t in enumerate(live)}
    slot_y = {t: n + 5 for n, t in enumerate(t for t in live if pieces[t][1] == "t")}
    slot_y.update({t: pieces[t][0] for t in live if pieces[t][1] == "g"})
    parity = lax.rem(me, 2)
    pair = me + 1 - 2 * parity

    def weight_slot(owner_router, owner_group, owner_parity, t):
        p, kind, start, length = pieces[t]
        index = {
            "t": owner_group * 2 + owner_parity,
            "g": owner_group,
            "p": owner_parity,
            "o": 0,
        }[kind]
        start = start + index * length
        if kind != "o":
            start = pl.multiple_of(start, 16)
        span = pl.ds(start, length)
        if p < 4:
            return w_all.at[p, owner_router, span, :]
        return wo_all.at[owner_router, span, :]

    def piece_bytes(t):
        return size(weight_slot(0, 0, 0, t))

    def x_copy(j, t, source_router):
        spot = weight_slot(source_router, g, parity, t)
        return pltpu.make_async_remote_copy(
            src_ref=spot,
            dst_ref=spot,
            send_sem=sent.at[0],
            recv_sem=x_recv.at[j - 1, slot_x[t]],
            device_id={"routers": lax.rem(r + j, routers)},
            device_id_type=MESH,
        )

    def y_copy(i, j, t, owner_group):
        spot = weight_slot(lax.rem(r - j + routers, routers), owner_group, parity, t)
        return pltpu.make_async_remote_copy(
            src_ref=spot,
            dst_ref=spot,
            send_sem=sent.at[0],
            recv_sem=y_recv.at[i - 1, j - 1, slot_y[t]],
            device_id={"groups": lax.rem(g + i, groups)},
            device_id_type=MESH,
        )

    def pair_copy(i, j, t):
        spot = weight_slot(
            lax.rem(r - j + routers, routers), lax.rem(g - i + groups, groups), parity, t
        )
        return pltpu.make_async_remote_copy(
            src_ref=spot,
            dst_ref=spot,
            send_sem=sent.at[0],
            recv_sem=w_recv.at[j - 1, pieces[t][0]],
            device_id={"users": pair},
            device_id_type=MESH,
        )

    def send_x(t):
        if t in live:
            for j in range(1, routers):
                x_copy(j, t, r).start()

    def send_first():
        lead[0].wait()
        for t in range(opening):
            if order[t] != ahead[0] and ahead[1] not in order[:t]:
                lead[1].wait()
            send_x(t)

    send_first()
    for c in first[:3]:
        c.wait()
    owners = [owner_ref[b] for b in range(blocks)]
    ranks = []
    for b in range(blocks):
        rank = jnp.int32(0)
        for a in range(b):
            rank = rank + jnp.where(owners[a] == owners[b], 1, 0)
        ranks.append(rank)

    def slot_source(dest, cap):
        index, user = jnp.int32(0), jnp.int32(-1)
        for b in range(blocks):
            hit = (owners[b] == dest) & (ranks[b] == cap)
            index = jnp.where(hit, b, index)
            user = jnp.where(hit, user_ref[b], user)
        return index, user

    mask_bytes = size(mask_out) // users
    slot_bytes = size(out_slots) // users
    cached = keys_v.shape[0]
    row_user = lax.broadcasted_iota(jnp.int32, (8, HEAD_DIM), 0)
    mask_copies, item_copies = {}, {}

    def across(k):
        other = me
        bit = 1
        while bit < users:
            if k & bit:
                other = other + bit - 2 * bit * lax.rem(me // bit, 2)
            bit *= 2
        return other

    def z_copy(k, source):
        return pltpu.make_async_remote_copy(
            src_ref=out_slots.at[k],
            dst_ref=x_all.at[pl.ds(source * CAP, CAP), pl.ds(pl.multiple_of(h * wh, wh), wh), :],
            send_sem=sent.at[0],
            recv_sem=z_recv.at[k - 1],
            device_id={"users": across(k)},
            device_id_type=MESH,
        )

    def m_copy(k, source):
        return pltpu.make_async_remote_copy(
            src_ref=mask_out.at[k],
            dst_ref=mask_all.at[source],
            send_sem=sent.at[0],
            recv_sem=group_recv.at[0],
            device_id={"users": across(k)},
            device_id_type=MESH,
        )

    def relay_copy(k, part):
        spot = x_all.at[
            pl.ds(across(k) * CAP, CAP), pl.ds(pl.multiple_of(part * wh, wh), wh), :
        ]
        return pltpu.make_async_remote_copy(
            src_ref=spot,
            dst_ref=spot,
            send_sem=sent.at[0],
            recv_sem=group_recv.at[2 if k == 1 else 1],
            device_id={"heads": mate},
            device_id_type=MESH,
        )

    for k in list(range(1, users)) + [0]:
        lines = jnp.zeros((8, HEAD_DIM), F32)
        for cap in range(CAP):
            user = slot_source(across(k), cap)[1]
            lines = lines + jnp.where(row_user == user + cap * cached, jnp.where(user < 0, 0.0, 1.0), 0.0)
        if k:
            mask_out[k] = lines
            m_copy(k, me).start()
        else:
            mask_all[me] = lines
    first[3].wait()
    for k in list(range(1, users)) + [0]:
        for cap in range(CAP):
            index = slot_source(across(k), cap)[0]
            if k:
                out_slots[k, cap] = items_v[index, pl.ds(pl.multiple_of(h * wh, wh), wh), :]
            else:
                x_all[me * CAP + cap] = items_v[index]
        if k:
            z_copy(k, me).start()
    drain(local_sem.at[7], size(w_o_ref) + len(later) * (size(w_in_ref) // 4))
    for t in range(opening, len(pieces)):
        send_x(t)
    for c in rest + gains:
        c.start()

    def forward(t):
        if t not in live:
            return
        kind = pieces[t][1]
        for j in range(1, routers):
            x_copy(j, t, lax.rem(r - j + routers, routers)).wait_recv()
            if kind in "tg":
                for i in range(1, groups):
                    y_copy(i, j, t, g).start()
            if kind in "tp":
                pair_copy(0, j, t).start()

    def second(t):
        if t not in live:
            return
        for j in range(1, routers):
            for i in range(1, groups):
                y_copy(i, j, t, lax.rem(g - i + groups, groups)).wait_recv()
                pair_copy(i, j, t).start()

    def landed(p):
        mine_of = [t for t in live if pieces[t][0] == p]
        straight = sum(piece_bytes(t) for t in mine_of if pieces[t][1] == "g")
        paired = sum(
            piece_bytes(t) * (groups if pieces[t][1] == "t" else 1)
            for t in mine_of
            if pieces[t][1] in "tp"
        )
        for j in range(1, routers):
            for t in mine_of:
                if pieces[t][1] == "o":
                    x_copy(j, t, lax.rem(r - j + routers, routers)).wait_recv()
            for i in range(1, groups):
                if straight:
                    drain(y_recv.at[i - 1, j - 1, p], straight)
            if paired:
                drain(w_recv.at[j - 1, p], paired)

    tile_slots = 4
    tile = tile_slots * width

    wide = 2 * tile

    def wide_span(i):
        return pl.ds(pl.multiple_of(i * wide, wide), wide)

    def product(p, i, a):
        cols = pl.ds(pl.multiple_of(a * depth, depth), depth)
        x = x_all[pl.ds(i * 2 * tile_slots, 2 * tile_slots), :, cols]
        return jnp.dot(x.reshape(wide, depth), w_all[p, a], preferred_element_type=F32)

    def prepare(i, p):
        pre_v[p, wide_span(i), :] = product(p, i, r)

    def projected(p, i):
        total = pre_v[p, wide_span(i), :]
        for j in range(1, routers):
            total = total + product(p, i, lax.rem(r - j + routers, routers))
        return silu(total)

    def query(i):
        q_v[wide_span(i), :] = projected(0, i).astype(BF16)

    def turn():
        gain_v[...] = mlp_gain_ref[...].astype(F32).reshape(1, -1)
        for e in range(heads_here):
            for u in range(cached):
                turned[e, u * HEAD_DIM : (u + 1) * HEAD_DIM, :] = keys_v[
                    u, :, e * HEAD_DIM : (e + 1) * HEAD_DIM
                ].T

    def picking(i):
        for s in range(2 * tile_slots):
            for u in range(cached):
                spot = s % CAP * cached + u
                line = mask_all[i * (2 * tile_slots // CAP) + s // CAP, spot : spot + 1, :]
                rows_s = pl.ds(pl.multiple_of(i * wide + s * width, width), width)
                pick_v[u, rows_s, :] = jnp.broadcast_to(line, (width, HEAD_DIM)).astype(BF16)

    def attend(i, part):
        span = wide_span(i)
        picks = [pick_v[u, span, :] for u in range(cached)]
        share = heads_here // 2
        for e in range(part * share, (part + 1) * share):
            cols = slice(e * HEAD_DIM, (e + 1) * HEAD_DIM)
            q = q_v[span, cols]
            raw = jnp.dot(
                jnp.concatenate([q * pick for pick in picks], axis=1),
                turned[e],
                preferred_element_type=F32,
            )
            weights = silu(raw * scale).astype(BF16)
            times = per_user // HEAD_DIM
            weights = jnp.concatenate(
                [weights * jnp.concatenate([pick] * times, axis=1) for pick in picks], axis=1
            )
            att_v[span, cols] = (
                jnp.dot(
                    weights,
                    values_v[:, :, cols].reshape(positions, HEAD_DIM),
                    preferred_element_type=F32,
                )
                .astype(BF16)
                .astype(F32)
            )

    def self_key(i):
        span = wide_span(i)
        keys = projected(1, i)
        for e in range(heads_here):
            cols = slice(e * HEAD_DIM, (e + 1) * HEAD_DIM)
            own = jnp.sum(q_v[span, cols].astype(F32) * keys[:, cols], axis=1, keepdims=True)
            own_v[span, cols] = jnp.broadcast_to(silu(own * scale), (wide, HEAD_DIM))

    lane = lax.broadcasted_iota(jnp.int32, (width, 128), 1)

    def self_value(i):
        span = wide_span(i)
        att = att_v[span, :] + own_v[span, :] * projected(2, i)
        att_v[span, :] = att
        total = jnp.sum(att, axis=1, keepdims=True)
        square = jnp.sum(att * att, axis=1, keepdims=True)
        packed = jnp.zeros((width, 128), F32)
        for b in range(wide // width):
            part = slice(b * width, (b + 1) * width)
            packed = jnp.where(lane == 2 * b, total[part], packed)
            packed = jnp.where(lane == 2 * b + 1, square[part], packed)
        stat_out[i] = packed

    def gate(i):
        gate_v[wide_span(i), :] = attn_gain_ref[...].astype(F32).reshape(1, -1) * projected(3, i)

    def gating(i):
        stat_copy(i).wait_recv()
        both = stat_out[i] + stat_in[i]
        for b in range(wide // width):
            span = pl.ds(pl.multiple_of(i * wide + b * width, width), width)
            mean = both[:, 2 * b : 2 * b + 1] / hd_all
            var = both[:, 2 * b + 1 : 2 * b + 2] / hd_all - mean * mean
            gated_v[span, :] = (
                (att_v[span, :] - mean) * lax.rsqrt(var + EPSILON) * gate_v[span, :]
            ).astype(BF16)

    def stat_copy(i):
        return pltpu.make_async_remote_copy(
            src_ref=stat_out.at[i],
            dst_ref=stat_in.at[i],
            send_sem=sent.at[0],
            recv_sem=st_recv.at[i],
            device_id={"heads": mate},
            device_id_type=MESH,
        )

    def value(i):
        self_value(i)
        stat_copy(i).start()

    def whole(fun):
        for i in range(rows // wide):
            fun(i)

    half = rows // heads

    mine = users // heads
    seat, seat_mate = heads - 1 - h, heads - 1 - mate
    piece = half // 2
    source_rows = CAP * width

    def far_first(e, i, amount):
        return jnp.where(me < e * mine + mine // 2, amount - 1 - i, i)

    def part_copy(j, c):
        spot = pl.ds(pl.multiple_of(c * piece, piece), piece)
        return pltpu.make_async_remote_copy(
            src_ref=part_out.at[j, spot, :],
            dst_ref=part_in.at[j, spot, :],
            send_sem=sent.at[0],
            recv_sem=po_recv.at[c if j == 0 else 2 + c],
            device_id={"heads": mate},
            device_id_type=MESH,
        )

    def shares(j):
        pieces_of = (half,) if j == 0 else (piece, piece)
        for i, count in enumerate(pieces_of):
            c = 0 if j == 0 else far_first(seat_mate, i, 2)
            start = pl.multiple_of(c * piece, piece)
            part_out[j, pl.ds(start, count), :] = jnp.dot(
                gated_v[pl.ds(pl.multiple_of(seat_mate * half + start, piece), count), :],
                wo_all[lax.rem(r - j + routers, routers)],
                preferred_element_type=F32,
            ).astype(BF16)
            if j:
                part_copy(j, c).start()
        if j == 0:
            for i in range(2):
                part_copy(j, far_first(seat_mate, i, 2)).start()

    def outer(js):
        for j in js:
            shares(j)
        for j in js:
            part_own[j] = jnp.dot(
                gated_v[pl.ds(pl.multiple_of(seat * half, half), half), :],
                wo_all[lax.rem(r - j + routers, routers)],
                preferred_element_type=F32,
            )

    def step(name):
        if name == "T":
            drain(local_sem.at[10], size(keys_ref, values_ref, w_one_ref))
            for c in gains:
                c.wait()
            turn()
        elif name[0] == "f":
            forward(int(name[1:]))
        elif name[0] == "z":
            second(int(name[1:]))
        elif name[0] == "L":
            landed(int(name[1:]))
        elif name[0] == "r" and name[1] in "AB":
            if name[1] == "A":
                drain(group_recv.at[2], slot_bytes)
                drain(group_recv.at[0], (users - 1) * mask_bytes)
                whole(picking)
            else:
                drain(group_recv.at[1], (users - 2) * slot_bytes)
        elif name[0] == "r":
            for k in range(int(name[1:]), users if name == "r3" else int(name[1:]) + 1):
                z_copy(k, across(k)).wait_recv()
                relay_copy(k, h).start()
        elif name[0] == "p":
            whole(functools.partial(prepare, p=int(name[1])))
        elif name[0] == "q":
            whole(query)
        elif name[0] == "a":
            whole(functools.partial(attend, part=int(name[1])))
        elif name[0] == "k":
            whole(self_key)
        elif name[0] == "v":
            whole(value)
        elif name == "g0":
            whole(gate)
        elif name == "g1":
            whole(gating)
        elif name == "o0":
            outer([0])
        else:
            outer(range(1, routers))

    for name in STEPS:
        with jax.named_scope(name):
            step(name)

    two = jnp.broadcast_to(
        w_two_ref[...].astype(F32).reshape(1, -1), (8, w_two_ref.shape[0])
    ).astype(BF16)

    def mixed(source, j):
        a = lax.rem(r - j + routers, routers)
        span = pl.ds(pl.multiple_of(source * source_rows, source_rows), source_rows)
        cols = pl.ds(pl.multiple_of(a * out_cols, out_cols), out_cols)
        x = x_all[pl.ds((seat * mine + source) * CAP, CAP), :, cols]
        x = x.reshape(source_rows, out_cols).astype(F32)
        residual = x + part_own[j, span, :] + part_in[j, span, :].astype(F32)
        square = jnp.sum(residual * residual, axis=1, keepdims=True)
        scaled = (residual * gain_v[:, cols]).astype(BF16)
        return square, jnp.dot(scaled, w_one_v[cols, :], preferred_element_type=F32)

    def score(source, i, square, total):
        for j in range(1, routers):
            more = mixed(source, j)
            square, total = square + more[0], total + more[1]
        norm = lax.rsqrt(square / model + EPSILON)
        hidden = silu(norm * total).astype(BF16)
        sc_out[i] = lax.dot_general(
            two, hidden, (((1,), (1,)), ((), ())), preferred_element_type=F32
        )

    def score_copy(i, e, owner, sem):
        return pltpu.make_async_remote_copy(
            src_ref=sc_out.at[i],
            dst_ref=ret.at[owner],
            send_sem=sc_send.at[0],
            recv_sem=sc_recv.at[0],
            device_id={"users": seat * mine + far_first(seat, i, mine), "heads": e},
            device_id_type=MESH,
        )

    group = mine // 2
    early = {}
    with jax.named_scope("early"):
        for i in range(mine):
            source = far_first(seat, i, mine)
            if i % group == 0:
                drain(po_recv.at[far_first(seat, i // group, 2)], piece * out_cols * 2)
            early[i] = mixed(source, 0)
    for i in range(mine):
        source = far_first(seat, i, mine)
        if i % group == 0:
            with jax.named_scope("partwait"):
                drain(
                    po_recv.at[2 + far_first(seat, i // group, 2)],
                    (routers - 1) * piece * out_cols * 2,
                )
        with jax.named_scope("score"):
            score(source, i, *early[i])
        target = seat * mine + source
        for e in range(heads):
            itself = (target == me) & (h == e)

            @pl.when(jnp.logical_not(itself))
            def _():
                score_copy(i, e, me, me).start()

            @pl.when(itself)
            def _():
                ret[me] = sc_out[i]

    rounds = {"t": 1 + (groups - 1) + groups, "g": groups, "p": 2, "o": 1}
    hops = sum(piece_bytes(t) * rounds[pieces[t][1]] for t in live)
    total = (routers - 1) * hops + (users - 1) * (2 * slot_bytes + mask_bytes)
    drain(sent.at[0], total + size(stat_out) + size(part_out))
    handler = heads - 1 - me // mine
    score_bytes = size(ret) // users

    def gather(less):
        drain(sc_recv.at[0], (users - less) * score_bytes)
        drain(sc_send.at[0], (users - less) * score_bytes)

    pl.when(h == handler)(functools.partial(gather, 1))
    pl.when(h != handler)(functools.partial(gather, 0))

    position = lax.broadcasted_iota(jnp.int32, (1, width), 1)
    for b in range(blocks):
        tile_in = ret[owners[b]]
        line = tile_in[0:1, 0:width]
        for cap in range(1, CAP):
            line = jnp.where(ranks[b] == cap, tile_in[0:1, cap * width : (cap + 1) * width], line)
        out_ref[b : b + 1, :] = jnp.where(position < fill_ref[b], line, 0.0)


def local(
    sizes,
    items,
    block_owner,
    block_user,
    block_fill,
    prefix_keys,
    prefix_values,
    w_in,
    attn_gain,
    w_o,
    mlp_gain,
    w_one,
    w_two,
):
    groups, users, routers, heads = sizes
    blocks, width, model = items.shape
    projections, depth, half_width = w_in.shape
    slots = users * CAP
    rows = slots * width
    half = rows // heads
    out_cols = w_o.shape[1]
    cached, per_user, _ = prefix_keys.shape
    positions = cached * per_user
    pieces = plan(groups, depth, half_width)
    live = sum(1 for piece in pieces if piece[3])
    trees = sum(1 for piece in pieces if piece[3] and piece[1] == "t")
    dma = pltpu.SemaphoreType.DMA
    yard_bytes = 2 * (
        (routers - 1) * (w_in.size + w_o.size)
        + (users - 1) * (2 * CAP * (width // heads) * model + 2 * 8 * HEAD_DIM)
        + 2 * 2 * rows * 128
        + routers * half * out_cols
    )
    yard_rows = yard_bytes // 256 // 8 * 8
    hbm = pl.BlockSpec(memory_space=pl.ANY)
    vmem = pl.BlockSpec(memory_space=pltpu.VMEM)
    scratch = [
        pltpu.SMEM((blocks,), jnp.int32),
        pltpu.SMEM((blocks,), jnp.int32),
        pltpu.SMEM((blocks,), jnp.int32),
        pltpu.VMEM(attn_gain.shape, BF16),
        pltpu.VMEM(mlp_gain.shape, BF16),
        pltpu.VMEM(w_two.shape, BF16),
        pltpu.VMEM((blocks, width, model), BF16),
        pltpu.VMEM((users, CAP, width // heads, model), BF16),
        pltpu.VMEM((slots, width, model), BF16),
        pltpu.VMEM((users, 8, HEAD_DIM), F32),
        pltpu.VMEM((users, 8, HEAD_DIM), F32),
        pltpu.VMEM(prefix_keys.shape, BF16),
        pltpu.VMEM(prefix_values.shape, BF16),
        pltpu.VMEM((half_width // HEAD_DIM, cached * HEAD_DIM, per_user), BF16),
        pltpu.VMEM((1, model), F32),
        pltpu.VMEM((cached, rows, HEAD_DIM), BF16),
        pltpu.VMEM((rows, half_width), F32),
        pltpu.VMEM((projections, rows, half_width), F32),
        pltpu.VMEM((projections, routers, depth, half_width), BF16),
        pltpu.VMEM((routers, half_width, out_cols), BF16),
        pltpu.VMEM(w_one.shape, BF16),
        pltpu.VMEM((rows, half_width), BF16),
        pltpu.VMEM((rows, half_width), F32),
        pltpu.VMEM((rows, half_width), F32),
        pltpu.VMEM((rows, half_width), BF16),
        pltpu.VMEM((rows // (8 * width), width, 128), F32),
        pltpu.VMEM((rows // (8 * width), width, 128), F32),
        pltpu.VMEM((routers, half, out_cols), BF16),
        pltpu.VMEM((routers, half, out_cols), F32),
        pltpu.VMEM((routers, half, out_cols), BF16),
        pltpu.VMEM((users // heads, 8, CAP * width), F32),
        pltpu.VMEM((users, 8, CAP * width), F32),
        dma((11,)),
        dma((1,)),
        dma((users - 1,)),
        dma((3,)),
        dma((routers - 1, live)),
        dma((groups - 1, routers - 1, 5 + trees)),
        dma((routers - 1, 5)),
        dma((rows // (8 * width),)),
        dma((4,)),
        dma((1,)),
        dma((1,)),
        pltpu.VMEM((yard_rows, 128), BF16),
    ]
    return pl.pallas_call(
        functools.partial(scorer, sizes),
        out_shape=pltpu.VMEM((blocks, width), F32),
        in_specs=[hbm] * 12,
        out_specs=vmem,
        scratch_shapes=scratch,
        compiler_params=pltpu.CompilerParams(
            collective_id=0, has_side_effects=True, vmem_limit_bytes=62 * 1024 * 1024
        ),
    )(
        items,
        block_owner.reshape(-1),
        block_user,
        block_fill,
        prefix_keys,
        prefix_values,
        w_in,
        attn_gain,
        w_o,
        mlp_gain,
        w_one,
        w_two,
    )


def solution(mesh):
    placed = (
        P(("groups", "users", "routers"), None, None),
        P(("groups", "users", "routers"), None),
        P(("groups", "users", "routers")),
        P(("groups", "users", "routers")),
        P(("groups", "users"), None, "heads"),
        P(("groups", "users"), None, "heads"),
        P(None, "routers", "heads"),
        P("heads"),
        P("heads", "routers"),
        P(),
        P(),
        P(),
    )
    sizes = tuple(mesh.shape[name] for name in ("groups", "users", "routers", "heads"))
    return jax.shard_map(
        functools.partial(local, sizes),
        mesh=mesh,
        in_specs=placed,
        out_specs=P(("groups", "users", "routers"), None),
        check_vma=False,
    )
```
